16 devices in a mesh: data: 16 (over z, y, x, core).
Axes of the slice: x: 2, y: 2, z: 2, core: 2. Of those that a mesh axis runs over, the one named last changes fastest.
Arguments:
- tokens: bfloat16 [131072, 128], P('data')
- out_grad: bfloat16 [131072, 128], P('data')
- w_up: bfloat16 [2, 128, 512], replicated
- w_down: bfloat16 [2, 512, 128], replicated
- a_up_old: float32 [2, 128, 128], replicated
- s_up_old: float32 [2, 512, 512], replicated
- a_down_old: float32 [2, 512, 512], replicated
- s_down_old: float32 [2, 128, 128], replicated
- a_up_inv: float32 [2, 128, 128], replicated
- s_up_inv: float32 [2, 512, 512], replicated
- a_down_inv: float32 [2, 512, 512], replicated
- s_down_inv: float32 [2, 128, 128], replicated
- factor_decay: float32 [], replicated
Outputs:
- output 1: float32 [2, 128, 512], replicated
- output 2: float32 [2, 512, 128], replicated
- output 3: float32 [2, 128, 128], replicated
- output 4: float32 [2, 512, 512], replicated
- output 5: float32 [2, 512, 512], replicated
- output 6: float32 [2, 128, 128], replicated
All inputs are finite; a program needn't handle non-finite values.
Results may differ from the reference program's by a relative error of at most 0.00179582.
Values are sent between devices in bfloat16 or wider.
A program may use at most 1 GiB of HBM per device.

```python
import math
import jax
import jax.numpy as jnp
from jax import lax

D = 128
FF = 512
TOK_DEV = 8192
SHARDS = 16
BLOCKS = 2


def gelu_fn(pre_act):
    return jax.nn.gelu(pre_act, approximate=True)


def spd_draw(rng_key, width, diag_low, diag_high):
    key_diag, key_low = jax.random.split(rng_key)
    diag_part = jax.random.uniform(key_diag, (BLOCKS, width), jnp.float32, diag_low, diag_high)
    low_rank = jax.random.normal(key_low, (BLOCKS, width, 64), jnp.float32)
    outer_part = jnp.einsum("bik,bjk->bij", low_rank, low_rank) / math.sqrt(width * 64.0)
    return outer_part + diag_part[:, :, None] * jnp.eye(width, dtype=jnp.float32)[None]


def shifted_rows(key_scale, key_shift, key_noise):
    row_scale = jnp.exp(1.5 * jax.random.uniform(key_scale, (SHARDS, 1, 1), jnp.float32, -1.0, 1.0))
    row_shift = 0.7 * jax.random.normal(key_shift, (SHARDS, 1, D), jnp.float32)
    row_noise = jax.random.normal(key_noise, (SHARDS, TOK_DEV, D), jnp.float32)
    return (row_noise * row_scale + row_shift).reshape(SHARDS * TOK_DEV, D).astype(jnp.bfloat16)


def setup_inputs(seed: int = 0) -> dict:
    sub_keys = jax.random.split(jax.random.key(seed), 17)
    w_up = jax.random.normal(sub_keys[6], (BLOCKS, D, FF), jnp.float32) / math.sqrt(D)
    w_down = jax.random.normal(sub_keys[7], (BLOCKS, FF, D), jnp.float32) / math.sqrt(FF)
    return {
        "tokens": shifted_rows(sub_keys[0], sub_keys[1], sub_keys[2]),
        "out_grad": shifted_rows(sub_keys[3], sub_keys[4], sub_keys[5]),
        "w_up": w_up.astype(jnp.bfloat16),
        "w_down": w_down.astype(jnp.bfloat16),
        "a_up_old": 0.3 * spd_draw(sub_keys[8], D, 0.5, 1.5),
        "s_up_old": 0.3 * spd_draw(sub_keys[9], FF, 0.5, 1.5),
        "a_down_old": 0.3 * spd_draw(sub_keys[10], FF, 0.5, 1.5),
        "s_down_old": 0.3 * spd_draw(sub_keys[11], D, 0.5, 1.5),
        "a_up_inv": spd_draw(sub_keys[12], D, 0.5, 1.5),
        "s_up_inv": spd_draw(sub_keys[13], FF, 0.5, 1.5),
        "a_down_inv": spd_draw(sub_keys[14], FF, 0.5, 1.5),
        "s_down_inv": spd_draw(sub_keys[15], D, 0.5, 1.5),
        "factor_decay": jax.random.uniform(sub_keys[16], (), jnp.float32, 0.6, 0.9),
    }


def cross_sum(left, right):
    return jnp.dot(left.T, right, preferred_element_type=jnp.float32)


def reference(tokens, out_grad, w_up, w_down, a_up_old, s_up_old, a_down_old, s_down_old,
              a_up_inv, s_up_inv, a_down_inv, s_down_inv, factor_decay):
    batch_total = SHARDS * TOK_DEV

    def shard_step(carry, rows_pair):
        tok_rows, grad_rows = rows_pair
        layer_ins = []
        pre_ups = []
        hiddens = []
        layer_in = tok_rows
        for block_idx in range(BLOCKS):
            pre_up = jnp.dot(layer_in, w_up[block_idx], preferred_element_type=jnp.float32).astype(jnp.bfloat16)
            hidden = gelu_fn(pre_up.astype(jnp.float32)).astype(jnp.bfloat16)
            layer_ins.append(layer_in)
            pre_ups.append(pre_up)
            hiddens.append(hidden)
            if block_idx + 1 < BLOCKS:
                layer_in = jnp.dot(hidden, w_down[block_idx], preferred_element_type=jnp.float32).astype(jnp.bfloat16)
        found = [[], [], [], [], [], []]
        grad_down = grad_rows
        for block_idx in reversed(range(BLOCKS)):
            hidden = hiddens[block_idx]
            layer_in = layer_ins[block_idx]
            d_hidden = jnp.dot(grad_down, w_down[block_idx].T, preferred_element_type=jnp.float32).astype(jnp.bfloat16)
            gelu_back = jax.vjp(gelu_fn, pre_ups[block_idx].astype(jnp.float32))[1]
            grad_up = gelu_back(d_hidden.astype(jnp.float32))[0].astype(jnp.bfloat16)
            terms = (cross_sum(layer_in, grad_up), cross_sum(hidden, grad_down),
                     cross_sum(layer_in, layer_in), cross_sum(grad_up, grad_up),
                     cross_sum(hidden, hidden), cross_sum(grad_down, grad_down))
            for slot, term in enumerate(terms):
                found[slot].insert(0, term)
            if block_idx > 0:
                grad_down = jnp.dot(grad_up, w_up[block_idx].T, preferred_element_type=jnp.float32).astype(jnp.bfloat16)
        return tuple(acc_sum + jnp.stack(items) for acc_sum, items in zip(carry, found)), None

    zero_init = (jnp.zeros((BLOCKS, D, FF), jnp.float32), jnp.zeros((BLOCKS, FF, D), jnp.float32),
                 jnp.zeros((BLOCKS, D, D), jnp.float32), jnp.zeros((BLOCKS, FF, FF), jnp.float32),
                 jnp.zeros((BLOCKS, FF, FF), jnp.float32), jnp.zeros((BLOCKS, D, D), jnp.float32))
    rows_in = (tokens.reshape(SHARDS, TOK_DEV, D), out_grad.reshape(SHARDS, TOK_DEV, D))
    totals = lax.scan(shard_step, zero_init, rows_in)[0]
    dw_up, dw_down, a_up, s_up, a_down, s_down = [total / batch_total for total in totals]
    decay_keep = factor_decay
    decay_fresh = 1.0 - factor_decay
    a_up_new = decay_keep * a_up_old + decay_fresh * a_up
    s_up_new = decay_keep * s_up_old + decay_fresh * s_up
    a_down_new = decay_keep * a_down_old + decay_fresh * a_down
    s_down_new = decay_keep * s_down_old + decay_fresh * s_down
    precond_up = jnp.einsum("bij,bjk->bik", jnp.einsum("bij,bjk->bik", a_up_inv, dw_up), s_up_inv)
    precond_down = jnp.einsum("bij,bjk->bik", jnp.einsum("bij,bjk->bik", a_down_inv, dw_down), s_down_inv)
    return (precond_up, precond_down, a_up_new, s_up_new, a_down_new, s_down_new)
```

```python
import functools

import jax
import jax.numpy as jnp
from jax import lax
from jax.experimental import pallas as pl
from jax.experimental.pallas import tpu as pltpu
from jax.sharding import PartitionSpec as P

BF = jnp.bfloat16
F32 = jnp.float32
MESH = pl.DeviceIdType.MESH
HIGH = lax.Precision.HIGHEST
C0 = 0.7978845608028654
CA = C0 * 0.044715
TILE = 1024
PIECES = 6
ROWS = 1280
LENS = (640, 320, 160, 80)
RECV_OFF = (0, 640, 960, 1120)
STRIDE = {"c": 1, "x": 2, "y": 4, "z": 8}
ORDERS = ("cxyz", "cyzx", "czxy")
TRI = [(r, c) for c in range(5) for r in range(c, 5)]
SLOTS = {}
for _rc in [(4, c) for c in range(4)] + [(r, c) for r, c in TRI if not (r == 4 and c < 4)]:
    for _k in range(4):
        SLOTS[(_k,) + _rc] = len(SLOTS)


def mm(a, b):
    return lax.dot_general(a, b, (((1,), (0,)), ((), ())), preferred_element_type=F32)


def nt(a, b):
    return lax.dot_general(a, b, (((1,), (1,)), ((), ())), preferred_element_type=F32)


def fine(a, b, ca, cb):
    return lax.dot_general(a, b, (((ca,), (cb,)), ((), ())), precision=HIGH, preferred_element_type=F32)


def gelu_pair(z):
    sq = z * z
    cub = CA * sq
    base = cub + C0
    half = 0.5 * jnp.tanh(z * base) + 0.5
    hid = z * half
    slope = half + hid * ((base + (cub + cub)) * (2.0 - (half + half)))
    return hid, slope


def local_sums(tok, og, wu, wd, xs, us, wut, wdt, gp, acc0, acc1, acc2):
    u0 = tok[...].T
    q1 = og[...].T
    xs[0, 512:640, :] = u0
    us[0, 0:128, :] = u0
    xs[3, 512:640, :] = q1
    us[1, 128:256, :] = q1
    z0 = mm(wut[0], u0).astype(BF).astype(F32)
    hid, slope = gelu_pair(z0)
    xs[1, 0:512, :] = hid.astype(BF)
    gp[...] = slope
    u1 = mm(wdt[...], xs[1, 0:512, :]).astype(BF)
    xs[2, 512:640, :] = u1
    us[0, 128:256, :] = u1
    z1 = mm(wut[1], u1).astype(BF).astype(F32)
    d1 = mm(wd[1], q1).astype(BF).astype(F32)
    hid, slope = gelu_pair(z1)
    xs[3, 0:512, :] = hid.astype(BF)
    xs[2, 0:512, :] = (d1 * slope).astype(BF)
    q0 = mm(wu[1], xs[2, 0:512, :]).astype(BF)
    xs[1, 512:640, :] = q0
    us[1, 0:128, :] = q0
    d0 = mm(wd[0], q0).astype(BF).astype(F32)
    xs[0, 0:512, :] = (d0 * gp[...]).astype(BF)
    for k in range(4):
        acc0[k] += nt(xs[k], xs[k, 0:256, :])
        acc1[k] += nt(xs[k, 256:640, :], xs[k, 256:512, :])
    for k in range(2):
        acc2[k] += nt(us[k], us[k])


def pick(k, r, c, acc0, acc1, acc2):
    if c < 2:
        return acc0[k, 128 * r:128 * r + 128, 128 * c:128 * c + 128]
    if c < 4:
        return acc1[k, 128 * r - 256:128 * r - 128, 128 * c - 256:128 * c - 128]
    at = 128 * (k // 2)
    return acc2[k % 2, at:at + 128, at:at + 128]


def kernel(steps, axis_size, tok, og, wu, wd, rho, old_hbm, inv_hbm, outs, xs, us, wut, wdt, gp, acc0, acc1, acc2,
           part, recv, total, olds, invs, res, local_sem, send_sem, recv_sem):
    i = pl.program_id(0)
    me = lax.axis_index("data")
    bit = {d: (me // s) % 2 for d, s in STRIDE.items()}
    peer = {d: me + s - 2 * s * bit[d] for d, s in STRIDE.items()}
    loads = [pltpu.make_async_copy(src, dst, local_sem.at[n])
             for n, (src, dst) in enumerate(zip(tuple(old_hbm) + tuple(inv_hbm), tuple(olds) + tuple(invs)))]

    @pl.when(i == 0)
    def _():
        barrier = pltpu.get_barrier_semaphore()
        for d in "cxyz":
            pl.semaphore_signal(barrier, inc=1, device_id=(peer[d],), device_id_type=MESH)
        for load in loads:
            load.start()
        wut[0] = wu[0].T
        wut[1] = wu[1].T
        wdt[...] = wd[0].T
        acc0[...] = jnp.zeros_like(acc0)
        acc1[...] = jnp.zeros_like(acc1)
        acc2[...] = jnp.zeros_like(acc2)

    local_sums(tok, og, wu, wd, xs, us, wut, wdt, gp, acc0, acc1, acc2)

    @pl.when(i == steps - 1)
    def _():
        scale = 1.0 / (axis_size * steps * TILE)
        for (k, r, c), slot in SLOTS.items():
            piece, at = slot // 10, 128 * (slot % 10)
            part[piece, at:at + 128, :] = pick(k, r, c, acc0, acc1, acc2) * scale
        pl.semaphore_wait(pltpu.get_barrier_semaphore(), 4)

        def spot(piece, stage):
            at = 0
            for s in range(stage):
                at = at + bit[ORDERS[piece % 3][s]] * LENS[s]
            return at

        def halving(piece, stage):
            d = ORDERS[piece % 3][stage]
            size = LENS[stage]
            away = pl.multiple_of(spot(piece, stage) + (1 - bit[d]) * size, 8)
            return pltpu.make_async_remote_copy(
                src_ref=part.at[piece, pl.ds(away, size), :],
                dst_ref=recv.at[piece, pl.ds(RECV_OFF[stage], size), :],
                send_sem=send_sem.at[0, stage, piece], recv_sem=recv_sem.at[0, stage, piece],
                device_id=(peer[d],), device_id_type=MESH)

        def doubling(piece, stage):
            d = ORDERS[piece % 3][stage]
            size = LENS[stage]
            at = pl.multiple_of(spot(piece, stage + 1), 8)
            return pltpu.make_async_remote_copy(
                src_ref=total.at[piece, pl.ds(at, size), :],
                dst_ref=total.at[piece, pl.ds(at, size), :],
                send_sem=send_sem.at[1, stage, piece], recv_sem=recv_sem.at[1, stage, piece],
                device_id=(peer[d],), device_id_type=MESH)

        for piece in range(PIECES):
            halving(piece, 0).start()
        for stage in range(4):
            size = LENS[stage]
            for piece in range(PIECES):
                halving(piece, stage).wait_recv()
                at = spot(piece, stage + 1)
                if stage == 3:
                    here = pl.ds(pl.multiple_of(at, 8), size)
                    total[piece, here, :] = part[piece, here, :] + recv[piece, RECV_OFF[3]:RECV_OFF[3] + size, :]
                    doubling(piece, 3).start()
                    continue
                half = LENS[stage + 1]
                keep = bit[ORDERS[piece % 3][stage + 1]] * half
                for shift in (half - keep, keep):
                    here = pl.ds(pl.multiple_of(at + shift, 8), half)
                    there = pl.ds(pl.multiple_of(RECV_OFF[stage] + shift, 8), half)
                    part[piece, here, :] = part[piece, here, :] + recv[piece, there, :]
                halving(piece, stage + 1).start()
        for stage in (3, 2, 1, 0):
            for piece in range(PIECES):
                doubling(piece, stage).wait_recv()
                if stage:
                    doubling(piece, stage - 1).start()
        for stage in range(4):
            for piece in range(PIECES):
                halving(piece, stage).wait_send()
                doubling(piece, stage).wait_send()

        for load in loads:
            load.wait()
        keep = rho[0]
        fresh = 1.0 - keep

        def block(k, r, c):
            slot = SLOTS[(k, r, c)]
            return total[slot // 10, 128 * (slot % 10):128 * (slot % 10) + 128, :]

        def blend(n, b, r, c, value):
            rows, cols = slice(128 * r, 128 * r + 128), slice(128 * c, 128 * c + 128)
            res[n][b, rows, cols] = keep * olds[n - 2][b, rows, cols] + fresh * value

        for b in range(2):
            for wide, narrow, k in ((3, 2, 2 * b), (4, 5, 2 * b + 1)):
                for c in range(4):
                    for r in range(c, 4):
                        value = block(k, r, c)
                        blend(wide, b, r, c, value)
                        if r > c:
                            blend(wide, b, c, r, value.T)
                blend(narrow, b, 0, 0, block(k, 4, 4))
            grad = jnp.concatenate([block(2 * b, 4, c) for c in range(4)], axis=1)
            res[0][b] = fine(fine(invs[0][b], grad, 1, 0), invs[1][b], 1, 0)
            grad = jnp.concatenate([block(2 * b + 1, 4, c) for c in range(4)], axis=1)
            res[1][b] = fine(invs[3][b], fine(grad, invs[2][b], 1, 1), 0, 0).T
        stores = [pltpu.make_async_copy(src, dst, local_sem.at[8 + n]) for n, (src, dst) in enumerate(zip(res, outs))]
        for store in stores:
            store.start()
        for store in stores:
            store.wait()


def solution(mesh):
    axis_size = mesh.shape["data"]

    def local_step(tokens, out_grad, w_up, w_down, a_up_old, s_up_old, a_down_old, s_down_old,
                   a_up_inv, s_up_inv, a_down_inv, s_down_inv, factor_decay):
        steps = tokens.shape[0] // TILE
        small, wide = (2, 128, 128), (2, 512, 512)
        out_shapes = ((2, 128, 512), (2, 512, 128), small, wide, wide, small)

        def body(tok, og, wu, wd, rho, *refs):
            kernel(steps, axis_size, tok, og, wu, wd, rho, refs[0:4], refs[4:8], refs[8:14], *refs[14:25],
                   refs[25:29], refs[29:33], refs[33:39], *refs[39:])

        fixed = lambda *shape: pl.BlockSpec(shape, lambda i: (0,) * len(shape))
        anywhere = pl.BlockSpec(memory_space=pl.ANY)
        vmem = lambda *shape: pltpu.VMEM(shape, F32)
        return pl.pallas_call(
            body,
            grid=(steps,),
            in_specs=[pl.BlockSpec((TILE, 128), lambda i: (i, 0))] * 2
            + [fixed(2, 128, 512), fixed(2, 512, 128), pl.BlockSpec(memory_space=pltpu.SMEM)] + [anywhere] * 8,
            out_specs=[anywhere] * 6,
            out_shape=[jax.ShapeDtypeStruct(s, F32) for s in out_shapes],
            scratch_shapes=[pltpu.VMEM((4, 640, TILE), BF), pltpu.VMEM((2, 256, TILE), BF), pltpu.VMEM((2, 512, 128), BF),
                            pltpu.VMEM((128, 512), BF), vmem(512, TILE), vmem(4, 640, 256), vmem(4, 384, 256),
                            vmem(2, 256, 256), vmem(PIECES, ROWS, 128), vmem(PIECES, 1200, 128), vmem(PIECES, ROWS, 128)]
            + [vmem(*s) for s in (small, wide, wide, small)] * 2 + [vmem(*s) for s in out_shapes]
            + [pltpu.SemaphoreType.DMA((14,)), pltpu.SemaphoreType.DMA((2, 4, PIECES)), pltpu.SemaphoreType.DMA((2, 4, PIECES))],
            compiler_params=pltpu.CompilerParams(dimension_semantics=("arbitrary",), vmem_limit_bytes=60 * 2**20,
                                                 collective_id=0, has_side_effects=True),
        )(tokens, out_grad, w_up, w_down, factor_decay.reshape(1), a_up_old, s_up_old, a_down_old, s_down_old,
          a_up_inv, s_up_inv, a_down_inv, s_down_inv)

    batch_spec = P("data", None)
    return jax.shard_map(local_step, mesh=mesh, in_specs=(batch_spec, batch_spec) + (P(),) * 11,
                         out_specs=(P(),) * 6, check_vma=False)
```

```python
import jax
import jax.numpy as jnp
from jax import lax
from jax.experimental import pallas as pl
from jax.experimental.pallas import tpu as pltpu
from jax.sharding import PartitionSpec as P

BF = jnp.bfloat16
F32 = jnp.float32
MESH = pl.DeviceIdType.MESH
HIGH = lax.Precision.HIGHEST
C0 = 0.7978845608028654
CA = C0 * 0.044715
TILE = 512
CHUNK = 256
STRIDE = {"c": 1, "x": 2, "y": 4, "z": 8}
ORDERS = ("cxyz", "cyzx", "czxy")

KEPT = {"S": [(r, c) for c in range(4) for r in range(c, 4)],
        "H": [(0, 0), (1, 0), (1, 1), (2, 2), (3, 2), (3, 3), (0, 2), (1, 2), (0, 3), (1, 3)]}


def tri(kind, b):
    return [(kind, b, r, c) for r, c in KEPT[kind]]


def row(kind, b):
    return [(kind, b, 0, c) for c in range(4)]


GROUPS = (
    (3, tri("H", 0)),
    (6, row("U", 1) + row("D", 1) + [("A", 1, 0, 0), ("Q", 1, 0, 0)] + tri("S", 1) + tri("H", 1)),
    (6, row("U", 0) + row("D", 0) + [("A", 0, 0, 0), ("Q", 0, 0, 0)] + tri("S", 0)),
)
SLOT = {}
PIECES = []
GROUP_PIECES = []
for _count, _blocks in GROUPS:
    _members = []
    for _n in range(_count):
        _size = -(-len(_blocks) // (_count - _n))
        _members.append(len(PIECES))
        PIECES.append((ORDERS[_n % 3], 128 * len(SLOT), 128 * _size))
        for _block in _blocks[:_size]:
            SLOT[_block] = 128 * len(SLOT)
        _blocks = _blocks[_size:]
    GROUP_PIECES.append(_members)
TOTAL_ROWS = 128 * len(SLOT)


def mm(a, b):
    return lax.dot_general(a, b, (((1,), (0,)), ((), ())), preferred_element_type=F32)


def nt(a, b):
    return lax.dot_general(a, b, (((1,), (1,)), ((), ())), preferred_element_type=F32)


def fine(a, b, ca, cb):
    return lax.dot_general(a, b, (((ca,), (cb,)), ((), ())), precision=HIGH, preferred_element_type=F32)


def rounded(x):
    return x.astype(BF).astype(F32)


def gelu_pair(z):
    sq = z * z
    cub = CA * sq
    base = cub + C0
    half = 0.5 * jnp.tanh(z * base) + 0.5
    hid = z * half
    slope = half + hid * ((base + (cub + cub)) * (2.0 - (half + half)))
    return hid, slope


def weave(first, second):
    done = 0
    for n, step in enumerate(first):
        step()
        while done < len(second) and (done + 1) * len(first) <= (n + 1) * len(second):
            second[done]()
            done += 1
    for step in second[done:]:
        step()


def body(axis_size, rows, tok_hbm, og_hbm, wu, wd, rho, old_hbm, inv_hbm, outs,
         tok, og, hid0, slope0, grad0, tiles, wut, wdt, acc_a, acc_b, acc_c, acc_d, part, recv, total, res,
         load_sem, out_sem, send_sem, recv_sem):
    me = lax.axis_index("data")
    bit = {d: (me // s) % 2 for d, s in STRIDE.items()}
    peer = {d: me + s - 2 * s * bit[d] for d, s in STRIDE.items()}
    count = rows // (2 * TILE)
    scale = 1.0 / (axis_size * rows)

    def tok_load(n):
        here = pl.ds(pl.multiple_of(n * (2 * TILE), 2 * TILE), 2 * TILE)
        return pltpu.make_async_copy(tok_hbm.at[here, :], tok.at[here, :], load_sem.at[n])

    og_load = pltpu.make_async_copy(og_hbm, og, load_sem.at[count])

    def place(n, b):
        if n % 4 in (1, 2):
            at = 512 * (4 * (n // 4) + 2 * (n % 4 - 1) + b)
            return slice(0, 512), slice(at, at + 512)
        at = 4096 + 128 * (4 * (n // 4) + 2 * (n % 4 == 3) + b)
        return slice(0, 128), slice(at, at + 128)

    late_loads = []
    for n, src in enumerate(tuple(old_hbm) + tuple(inv_hbm)):
        for b in range(2):
            at = place(n, b)
            late_loads.append(pltpu.make_async_copy(src.at[b], slope0.at[at[0], at[1]], load_sem.at[count + 1 + 2 * n + b]))

    def spot(piece, stage):
        order, base, size = PIECES[piece]
        at = base
        for s in range(stage):
            at = at + bit[order[s]] * (size >> (s + 1))
        return at

    def inbox(piece, stage):
        _, base, size = PIECES[piece]
        return base - base // 16 + sum(size >> (s + 1) for s in range(stage))

    def halving(piece, stage):
        order, _, size = PIECES[piece]
        half = size >> (stage + 1)
        away = pl.multiple_of(spot(piece, stage) + (1 - bit[order[stage]]) * half, 8)
        return pltpu.make_async_remote_copy(
            src_ref=part.at[pl.ds(away, half), :], dst_ref=recv.at[pl.ds(inbox(piece, stage), half), :],
            send_sem=send_sem.at[0, stage, piece], recv_sem=recv_sem.at[0, stage, piece],
            device_id=(peer[order[stage]],), device_id_type=MESH)

    def doubling(piece, stage):
        order, _, size = PIECES[piece]
        half = size >> (stage + 1)
        at = pl.multiple_of(spot(piece, stage + 1), 8)
        return pltpu.make_async_remote_copy(
            src_ref=total.at[pl.ds(at, half), :], dst_ref=total.at[pl.ds(at, half), :],
            send_sem=send_sem.at[1, stage, piece], recv_sem=recv_sem.at[1, stage, piece],
            device_id=(peer[order[stage]],), device_id_type=MESH)

    def tick(group, step):
        for piece in GROUP_PIECES[group]:
            order, _, size = PIECES[piece]
            if step == 0:
                halving(piece, 0).start()
            elif step < 4:
                stage = step - 1
                halving(piece, stage).wait_recv()
                at, box, half = spot(piece, step), inbox(piece, stage), size >> (step + 1)
                keep = bit[order[step]] * half
                for shift in (half - keep, keep):
                    here = pl.ds(pl.multiple_of(at + shift, 8), half)
                    there = pl.ds(pl.multiple_of(box + shift, 8), half)
                    part[here, :] = part[here, :] + recv[there, :]
                halving(piece, step).start()
            elif step == 4:
                halving(piece, 3).wait_recv()
                box, half = inbox(piece, 3), size >> 4
                here = pl.ds(pl.multiple_of(spot(piece, 4), 8), half)
                total[here, :] = part[here, :] + recv[box:box + half, :]
                doubling(piece, 3).start()
            else:
                doubling(piece, 8 - step).wait_recv()
                if step < 8:
                    doubling(piece, 7 - step).start()

    def near(n):
        return pl.ds(pl.multiple_of(n * TILE, TILE), TILE)

    def acts0(tile, n):
        kept = {}

        def start():
            kept["u"] = tok[near(n), :].T

        def chunk(f):
            def step():
                hid, slope = gelu_pair(rounded(mm(wut[0, f:f + CHUNK, :], kept["u"])))
                hid = hid.astype(BF)
                tile[768 + f:768 + f + CHUNK, :] = hid
                hid0[f:f + CHUNK, near(n)] = hid
                slope0[f:f + CHUNK, near(n)] = slope
            return step

        return [start] + [chunk(f) for f in range(0, 512, CHUNK)]

    def sums0(tile):
        def one():
            acc_a[0, 0:512, :] += nt(tile[768:1280, :], tile[1024:1280, :])

        def two():
            acc_b[0, 0:256, :] += nt(tile[768:1024, :], tile[768:1024, :])

        return [one, two]

    def acts1(tile, n):
        kept = {}

        def start():
            kept["q"] = og[near(n), :].T
            kept["u"] = mm(wdt[...], hid0[:, near(n)]).astype(BF)
            tile[512:640, :] = kept["u"]
            tile[640:768, :] = kept["q"]

        def chunk(f):
            def step():
                hid, slope = gelu_pair(rounded(mm(wut[1, f:f + CHUNK, :], kept["u"])))
                tile[768 + f:768 + f + CHUNK, :] = hid.astype(BF)
                tile[f:f + CHUNK, :] = (rounded(mm(wd[1, f:f + CHUNK, :], kept["q"])) * slope).astype(BF)
            return step

        def end():
            grad0[:, near(n)] = mm(wu[1], tile[0:512, :]).astype(BF)

        return [start] + [chunk(f) for f in range(0, 512, CHUNK)] + [end]

    def left_sums(tile, k):
        def one():
            acc_a[k] += nt(tile[0:640, :], tile[0:256, :])

        def two():
            acc_b[k] += nt(tile[256:640, :], tile[256:512, :])

        def three():
            acc_c[...] += nt(tile[512:768, :], tile[512:768, :])

        return [one, two, three]

    def sums1(tile):
        def one():
            acc_a[1] += nt(tile[640:1280, :], tile[1024:1280, :])

        def two():
            acc_b[1] += nt(tile[640:1024, :], tile[768:1024, :])

        return left_sums(tile, 0) + [one, two]

    def acts2(tile, n):
        kept = {}

        def start():
            tile[512:640, :] = tok[near(n), :].T
            tile[640:768, :] = grad0[:, near(n)]

        def chunk(f):
            def step():
                back = rounded(mm(wd[0, f:f + CHUNK, :], grad0[:, near(n)]))
                tile[f:f + CHUNK, :] = (back * slope0[f:f + CHUNK, near(n)]).astype(BF)
            return step

        return [start] + [chunk(f) for f in range(0, 512, CHUNK)]

    def sums2(tile, n):
        def one():
            acc_d[...] += nt(tile[640:768, :], hid0[:, near(n)])

        return left_sums(tile, 0) + [one]

    def phase(acts, sums, ticks):
        for acc in (acc_a, acc_b, acc_c, acc_d):
            acc[...] = jnp.zeros_like(acc)
        tiles[1][...] = jnp.zeros_like(tiles[1])

        def step(j, _):
            if acts is acts0:
                tok_load(j).wait()
            for side in range(2):
                n = 2 * j + side
                weave(acts(tiles[side], n), sums(tiles[1 - side], (n + 2 * count - 1) % (2 * count)))
            for when, group, what in ticks:
                @pl.when(j == when)
                def _():
                    tick(group, what)
            return 0

        lax.fori_loop(0, count, step, 0)
        for last in sums(tiles[1], 2 * count - 1):
            last()

    def put(block, value):
        part[SLOT[block]:SLOT[block] + 128, :] = value * scale

    def block_of(r, c):
        return slice(128 * r, 128 * r + 128), slice(128 * c, 128 * c + 128)

    def put_h(b, k, first):
        for r, c in KEPT["H"]:
            at = first + 128 * r
            put(("H", b, r, c), (acc_a if c > 1 else acc_b)[k, at:at + 128, 128 * (c % 2):128 * (c % 2) + 128])

    def put_left(b):
        for r, c in KEPT["S"]:
            rows_at, cols_at = block_of(r - 2 * (c > 1), c % 2)
            put(("S", b, r, c), (acc_b if c > 1 else acc_a)[0, rows_at, cols_at])
        for c in range(4):
            rows_at, cols_at = block_of(4 - 2 * (c > 1), c % 2)
            put(("U", b, 0, c), (acc_b if c > 1 else acc_a)[0, rows_at, cols_at])
        put(("A", b, 0, 0), acc_c[0:128, 0:128])
        put(("Q", b, 0, 0), acc_c[128:256, 128:256])

    barrier = pltpu.get_barrier_semaphore()
    for d in "cxyz":
        pl.semaphore_signal(barrier, inc=1, device_id=(peer[d],), device_id_type=MESH)
    for n in range(count):
        tok_load(n).start()
    og_load.start()
    wut[0] = wu[0].T
    wut[1] = wu[1].T
    wdt[...] = wd[0].T

    phase(acts0, lambda tile, n: sums0(tile), ())
    put_h(0, 0, 0)
    pl.semaphore_wait(barrier, 4)
    tick(0, 0)
    og_load.wait()

    phase(acts1, lambda tile, n: sums1(tile), ((0, 0, 1), (2, 0, 2), (3, 0, 3), (4, 0, 4), (5, 0, 5), (6, 0, 6), (7, 0, 7)))
    put_left(1)
    put_h(1, 1, 128)
    for c in range(4):
        acc = acc_a if c > 1 else acc_b
        put(("D", 1, 0, c), acc[1, 0:128, 128 * (c % 2):128 * (c % 2) + 128])
    tick(1, 0)
    tick(0, 8)

    phase(acts2, sums2, ((2, 1, 1), (6, 1, 2)))
    for load in late_loads:
        load.start()
    put_left(0)
    for c in range(4):
        put(("D", 0, 0, c), acc_d[:, 128 * c:128 * c + 128])
    tick(2, 0)

    keep = rho[0]
    fresh = 1.0 - keep

    def sum_of(block):
        return total[SLOT[block]:SLOT[block] + 128, :]

    def held(n, b):
        at = place(n, b)
        return slope0[at[0], at[1]]

    def blend(n, b, r, c, value):
        rows_at, cols_at = block_of(r, c)
        at = place(n, b)
        old = slope0[rows_at, at[1].start + 128 * c:at[1].start + 128 * c + 128]
        res[n + 2][b, rows_at, cols_at] = keep * old + fresh * value

    def symmetric(kind, n, b):
        for r, c in KEPT[kind]:
            value = sum_of((kind, b, r, c))
            blend(n, b, r, c, value)
            if r != c:
                blend(n, b, c, r, value.T)

    def precondition(b):
        grad = jnp.concatenate([sum_of(("U", b, 0, c)) for c in range(4)], axis=1)
        res[0][b] = fine(fine(held(4, b), grad, 1, 0), held(5, b), 1, 0)
        grad = jnp.concatenate([sum_of(("D", b, 0, c)) for c in range(4)], axis=1)
        res[1][b] = fine(held(7, b), fine(grad, held(6, b), 1, 1), 0, 0).T

    for step in range(1, 6):
        tick(1, step + 2)
        tick(2, step)
    tick(1, 8)
    tick(2, 6)
    for load in late_loads:
        load.wait()
    symmetric("H", 2, 0)
    tick(2, 7)
    blend(0, 1, 0, 0, sum_of(("A", 1, 0, 0)))
    blend(3, 1, 0, 0, sum_of(("Q", 1, 0, 0)))
    symmetric("S", 1, 1)
    symmetric("H", 2, 1)
    precondition(1)
    tick(2, 8)
    blend(0, 0, 0, 0, sum_of(("A", 0, 0, 0)))
    blend(3, 0, 0, 0, sum_of(("Q", 0, 0, 0)))
    symmetric("S", 1, 0)
    precondition(0)
    stores = [pltpu.make_async_copy(src, dst, out_sem.at[n]) for n, (src, dst) in enumerate(zip(res, outs))]
    for store in stores:
        store.start()
    for piece in range(len(PIECES)):
        for stage in range(4):
            halving(piece, stage).wait_send()
            doubling(piece, stage).wait_send()
    for store in stores:
        store.wait()


def solution(mesh):
    axis_size = mesh.shape["data"]

    def local_step(tokens, out_grad, w_up, w_down, a_up_old, s_up_old, a_down_old, s_down_old,
                   a_up_inv, s_up_inv, a_down_inv, s_down_inv, factor_decay):
        rows = tokens.shape[0]
        count = rows // (2 * TILE)
        small, wide = (2, 128, 128), (2, 512, 512)
        out_shapes = ((2, 128, 512), (2, 512, 128), small, wide, wide, small)

        def kernel(tok, og, wu, wd, rho, *refs):
            body(axis_size, rows, tok, og, wu, wd, rho, refs[0:4], refs[4:8], refs[8:14],
                 *refs[14:19], refs[19:21], *refs[21:30], refs[30:36], *refs[36:])

        anywhere = pl.BlockSpec(memory_space=pl.ANY)
        inside = pl.BlockSpec(memory_space=pltpu.VMEM)
        half = lambda *shape: pltpu.VMEM(shape, BF)
        full = lambda *shape: pltpu.VMEM(shape, F32)
        sems = pltpu.SemaphoreType.DMA
        return tuple(pl.pallas_call(
            kernel,
            in_specs=[anywhere] * 2 + [inside] * 2 + [pl.BlockSpec(memory_space=pltpu.SMEM)] + [anywhere] * 8,
            out_specs=[anywhere] * 6,
            out_shape=[jax.ShapeDtypeStruct(s, F32) for s in out_shapes],
            scratch_shapes=[half(rows, 128), half(rows, 128), half(512, rows), full(512, rows), half(128, rows),
                            half(1280, TILE), half(1280, TILE), half(2, 512, 128), half(128, 512),
                            full(2, 640, 256), full(2, 384, 256), full(256, 256), full(128, 512),
                            full(TOTAL_ROWS, 128), full(TOTAL_ROWS - TOTAL_ROWS // 16, 128), full(TOTAL_ROWS, 128)]
            + [full(*s) for s in out_shapes]
            + [sems((count + 17,)), sems((6,)), sems((2, 4, len(PIECES))), sems((2, 4, len(PIECES)))],
            compiler_params=pltpu.CompilerParams(vmem_limit_bytes=63 * 2**20, collective_id=0, has_side_effects=True),
        )(tokens, out_grad, w_up, w_down, factor_decay.reshape(1), a_up_old, s_up_old, a_down_old, s_down_old,
          a_up_inv, s_up_inv, a_down_inv, s_down_inv))

    batch_spec = P("data", None)
    return jax.shard_map(local_step, mesh=mesh, in_specs=(batch_spec, batch_spec) + (P(),) * 11,
                         out_specs=(P(),) * 6, check_vma=False)
```

```python
import jax
import jax.numpy as jnp
from jax import lax
from jax.experimental import pallas as pl
from jax.experimental.pallas import tpu as pltpu
from jax.sharding import PartitionSpec as P

BF = jnp.bfloat16
F32 = jnp.float32
MESH = pl.DeviceIdType.MESH
HIGH = lax.Precision.HIGHEST
C0 = 0.7978845608028654
CA = C0 * 0.044715
TILE = 512
CHUNK = 256
STRIDE = {"c": 1, "x": 2, "y": 4, "z": 8}
ORDERS = ("cxyz", "cyzx", "czxy")

LOWER = [(r, c) for c in range(4) for r in range(c, 4)]
MIXED = [(0, 0), (1, 0), (1, 1), (2, 2), (3, 2), (3, 3), (0, 2), (1, 2), (0, 3), (1, 3)]
KEPT = {("S", 0): LOWER, ("S", 1): LOWER, ("H", 0): LOWER, ("H", 1): MIXED}


def tri(kind, b):
    return [(kind, b, r, c) for r, c in KEPT[(kind, b)]]


def row(kind, b):
    return [(kind, b, 0, c) for c in range(4)]


GROUPS = (
    (6, row("D", 1) + [("A", 0, 0, 0), ("Q", 1, 0, 0)] + tri("H", 0) + tri("H", 1)),
    (6, row("U", 1) + row("D", 0) + [("A", 1, 0, 0), ("Q", 0, 0, 0)] + tri("S", 1)),
    (6, row("U", 0) + tri("S", 0)),
)
SLOT = {}
PIECES = []
GROUP_PIECES = []
for _count, _blocks in GROUPS:
    _members = []
    for _n in range(_count):
        _size = -(-len(_blocks) // (_count - _n))
        _members.append(len(PIECES))
        PIECES.append((ORDERS[_n % 3], 128 * len(SLOT), 128 * _size))
        for _block in _blocks[:_size]:
            SLOT[_block] = 128 * len(SLOT)
        _blocks = _blocks[_size:]
    GROUP_PIECES.append(_members)
TOTAL_ROWS = 128 * len(SLOT)


def mm(a, b):
    return lax.dot_general(a, b, (((1,), (0,)), ((), ())), preferred_element_type=F32)


def nt(a, b):
    return lax.dot_general(a, b, (((1,), (1,)), ((), ())), preferred_element_type=F32)


def fine(a, b, ca, cb):
    return lax.dot_general(a, b, (((ca,), (cb,)), ((), ())), precision=HIGH, preferred_element_type=F32)


def rounded(x):
    return x.astype(BF).astype(F32)


def gelu_parts(z):
    sq = z * z
    cub = CA * sq
    base = cub + C0
    half = 0.5 * jnp.tanh(z * base) + 0.5
    return cub, base, half


def gelu(z):
    return z * gelu_parts(z)[2]


def gelu_slope(z):
    cub, base, half = gelu_parts(z)
    return half + (z * half) * ((base + (cub + cub)) * (2.0 - (half + half)))


def weave(first, second):
    done = 0
    for n, step in enumerate(first):
        step()
        while done < len(second) and (done + 1) * len(first) <= (n + 1) * len(second):
            second[done]()
            done += 1
    for step in second[done:]:
        step()


def body(axis_size, rows, tok_hbm, og_hbm, wu, wd, rho, old_hbm, inv_hbm, outs,
         tok, og, pre0, pre1, hid0, mid, grad0, tiles, wut, wdt, acc_a, acc_b, acc_c, acc_d, part, recv, total, new, invs, res,
         load_sem, out_sem, send_sem, recv_sem):
    me = lax.axis_index("data")
    bit = {d: (me // s) % 2 for d, s in STRIDE.items()}
    peer = {d: me + s - 2 * s * bit[d] for d, s in STRIDE.items()}
    count = rows // (2 * TILE)
    scale = 1.0 / (axis_size * rows)

    def tok_load(n):
        here = pl.ds(pl.multiple_of(n * (2 * TILE), 2 * TILE), 2 * TILE)
        return pltpu.make_async_copy(tok_hbm.at[here, :], tok.at[here, :], load_sem.at[n])

    def og_load(n):
        here = pl.ds(pl.multiple_of(n * (2 * TILE), 2 * TILE), 2 * TILE)
        return pltpu.make_async_copy(og_hbm.at[here, :], og.at[here, :], load_sem.at[count + n])

    late_loads = [pltpu.make_async_copy(src, dst, load_sem.at[2 * count + n])
                  for n, (src, dst) in enumerate(zip(tuple(old_hbm) + tuple(inv_hbm), tuple(new) + tuple(invs)))]

    def spot(piece, stage):
        order, base, size = PIECES[piece]
        at = base
        for s in range(stage):
            at = at + bit[order[s]] * (size >> (s + 1))
        return at

    def inbox(piece, stage):
        _, base, size = PIECES[piece]
        return base - base // 16 + sum(size >> (s + 1) for s in range(stage))

    def halving(piece, stage):
        order, _, size = PIECES[piece]
        half = size >> (stage + 1)
        away = pl.multiple_of(spot(piece, stage) + (1 - bit[order[stage]]) * half, 8)
        return pltpu.make_async_remote_copy(
            src_ref=part.at[pl.ds(away, half), :], dst_ref=recv.at[pl.ds(inbox(piece, stage), half), :],
            send_sem=send_sem.at[0, stage, piece], recv_sem=recv_sem.at[0, stage, piece],
            device_id=(peer[order[stage]],), device_id_type=MESH)

    def doubling(piece, stage):
        order, _, size = PIECES[piece]
        half = size >> (stage + 1)
        at = pl.multiple_of(spot(piece, stage + 1), 8)
        return pltpu.make_async_remote_copy(
            src_ref=total.at[pl.ds(at, half), :], dst_ref=total.at[pl.ds(at, half), :],
            send_sem=send_sem.at[1, stage, piece], recv_sem=recv_sem.at[1, stage, piece],
            device_id=(peer[order[stage]],), device_id_type=MESH)

    def tick(group, step):
        for piece in GROUP_PIECES[group]:
            order, _, size = PIECES[piece]
            if step == 0:
                halving(piece, 0).start()
            elif step < 4:
                stage = step - 1
                halving(piece, stage).wait_recv()
                at, box, half = spot(piece, step), inbox(piece, stage), size >> (step + 1)
                keep = bit[order[step]] * half
                for shift in (half - keep, keep):
                    here = pl.ds(pl.multiple_of(at + shift, 8), half)
                    there = pl.ds(pl.multiple_of(box + shift, 8), half)
                    part[here, :] = part[here, :] + recv[there, :]
                halving(piece, step).start()
            elif step == 4:
                halving(piece, 3).wait_recv()
                box, half = inbox(piece, 3), size >> 4
                here = pl.ds(pl.multiple_of(spot(piece, 4), 8), half)
                total[here, :] = part[here, :] + recv[box:box + half, :]
                doubling(piece, 3).start()
            else:
                doubling(piece, 8 - step).wait_recv()
                if step < 8:
                    doubling(piece, 7 - step).start()

    def near(n):
        return pl.ds(pl.multiple_of(n * TILE, TILE), TILE)

    def chunks(make):
        return [make(f) for f in range(0, 512, CHUNK)]

    def acts0(tile, n):
        kept = {}

        def start():
            kept["u"] = tok[near(n), :].T
            tile[512:640, :] = kept["u"]
            tile[640:768, :] = og[near(n), :].T

        def first(f):
            def step():
                pre = mm(wut[0, f:f + CHUNK, :], kept["u"]).astype(BF)
                pre0[f:f + CHUNK, near(n)] = pre
                hid = gelu(pre.astype(F32)).astype(BF)
                tile[f:f + CHUNK, :] = hid
                hid0[f:f + CHUNK, near(n)] = hid
            return step

        def middle():
            kept["m"] = mm(wdt[...], tile[0:512, :]).astype(BF)
            mid[:, near(n)] = kept["m"]

        def second(f):
            def step():
                pre = mm(wut[1, f:f + CHUNK, :], kept["m"]).astype(BF)
                pre1[f:f + CHUNK, near(n)] = pre
                tile[768 + f:768 + f + CHUNK, :] = gelu(pre.astype(F32)).astype(BF)
            return step

        return [start] + chunks(first) + [middle] + chunks(second)

    def left_sums(tile, k, size):
        def one():
            acc_a[k, 0:size, :] += nt(tile[0:size, :], tile[0:256, :])

        def two():
            acc_b[k, 0:size - 256, :] += nt(tile[256:size, :], tile[256:512, :])

        return [one, two]

    def narrow_sums(tile):
        def one():
            acc_c[...] += nt(tile[512:768, :], tile[512:768, :])

        return [one]

    def sums0(tile, n):
        def one():
            acc_a[1] += nt(tile[640:1280, :], tile[1024:1280, :])

        def two():
            acc_b[1] += nt(tile[640:1024, :], tile[768:1024, :])

        return left_sums(tile, 0, 512) + narrow_sums(tile) + [one, two]

    def acts1(tile, n):
        kept = {}

        def start():
            kept["q"] = og[near(n), :].T
            tile[512:640, :] = mid[:, near(n)]

        def chunk(f):
            def step():
                back = rounded(mm(wd[1, f:f + CHUNK, :], kept["q"]))
                tile[f:f + CHUNK, :] = (back * gelu_slope(pre1[f:f + CHUNK, near(n)].astype(F32))).astype(BF)
            return step

        def end():
            grad = mm(wu[1], tile[0:512, :]).astype(BF)
            tile[640:768, :] = grad
            grad0[:, near(n)] = grad

        return [start] + chunks(chunk) + [end]

    def sums1(tile, n):
        def one():
            acc_d[...] += nt(tile[640:768, :], hid0[:, near(n)])

        return left_sums(tile, 0, 640) + narrow_sums(tile) + [one]

    def acts2(tile, n):
        def start():
            tile[512:640, :] = tok[near(n), :].T

        def chunk(f):
            def step():
                back = rounded(mm(wd[0, f:f + CHUNK, :], grad0[:, near(n)]))
                tile[f:f + CHUNK, :] = (back * gelu_slope(pre0[f:f + CHUNK, near(n)].astype(F32))).astype(BF)
            return step

        return [start] + chunks(chunk)

    def sums2(tile, n):
        return left_sums(tile, 0, 640)

    def phase(acts, sums, ticks):
        for acc in (acc_a, acc_b, acc_c, acc_d):
            acc[...] = jnp.zeros_like(acc)
        tiles[1][...] = jnp.zeros_like(tiles[1])

        def step(j, _):
            if acts is acts0:
                tok_load(j).wait()
                og_load(j).wait()
            for side in range(2):
                n = 2 * j + side
                weave(acts(tiles[side], n), sums(tiles[1 - side], (n + 2 * count - 1) % (2 * count)))
            for when, group, what in ticks:
                @pl.when(j == when)
                def _():
                    tick(group, what)
            return 0

        lax.fori_loop(0, count, step, 0)
        for last in sums(tiles[1], 2 * count - 1):
            last()

    def put(block, value):
        part[SLOT[block]:SLOT[block] + 128, :] = value * scale

    def block_of(r, c):
        return slice(128 * r, 128 * r + 128), slice(128 * c, 128 * c + 128)

    def put_left(kind, b):
        for r, c in LOWER:
            rows_at, cols_at = block_of(r - 2 * (c > 1), c % 2)
            put((kind, b, r, c), (acc_b if c > 1 else acc_a)[0, rows_at, cols_at])
        if kind == "S":
            for c in range(4):
                rows_at, cols_at = block_of(4 - 2 * (c > 1), c % 2)
                put(("U", b, 0, c), (acc_b if c > 1 else acc_a)[0, rows_at, cols_at])

    def put_right(b):
        for r, c in MIXED:
            rows_at, cols_at = block_of(r + 1, c % 2)
            put(("H", b, r, c), (acc_a if c > 1 else acc_b)[1, rows_at, cols_at])
        for c in range(4):
            rows_at, cols_at = block_of(0, c % 2)
            put(("D", b, 0, c), (acc_a if c > 1 else acc_b)[1, rows_at, cols_at])

    barrier = pltpu.get_barrier_semaphore()
    for d in "cxyz":
        pl.semaphore_signal(barrier, inc=1, device_id=(peer[d],), device_id_type=MESH)
    for n in range(count):
        tok_load(n).start()
        og_load(n).start()
    for load in late_loads:
        load.start()
    wut[0] = wu[0].T
    wut[1] = wu[1].T
    wdt[...] = wd[0].T

    phase(acts0, sums0, ())
    put_left("H", 0)
    put_right(1)
    put(("A", 0, 0, 0), acc_c[0:128, 0:128])
    put(("Q", 1, 0, 0), acc_c[128:256, 128:256])
    pl.semaphore_wait(barrier, 4)
    tick(0, 0)

    phase(acts1, sums1, ((1, 0, 1), (5, 0, 2)))
    put_left("S", 1)
    put(("A", 1, 0, 0), acc_c[0:128, 0:128])
    put(("Q", 0, 0, 0), acc_c[128:256, 128:256])
    for c in range(4):
        put(("D", 0, 0, c), acc_d[:, 128 * c:128 * c + 128])
    tick(1, 0)
    tick(0, 3)

    phase(acts2, sums2, ((1, 1, 1), (2, 0, 4), (4, 0, 5), (5, 1, 2), (7, 0, 6)))
    put_left("S", 0)
    tick(2, 0)

    keep = rho[0]
    fresh = 1.0 - keep

    for load in late_loads:
        load.wait()

    def sum_of(block):
        return total[SLOT[block]:SLOT[block] + 128, :]

    def blend(n, b, r, c, value):
        rows_at, cols_at = block_of(r, c)
        new[n][b, rows_at, cols_at] = keep * new[n][b, rows_at, cols_at] + fresh * value

    def symmetric(kind, n, b):
        for r, c in KEPT[(kind, b)]:
            value = sum_of((kind, b, r, c))
            blend(n, b, r, c, value)
            if r != c:
                blend(n, b, c, r, value.T)

    def narrow(kind, n, b):
        blend(n, b, 0, 0, sum_of((kind, b, 0, 0)))

    def precondition_up(b):
        grad = jnp.concatenate([sum_of(("U", b, 0, c)) for c in range(4)], axis=1)
        res[0][b] = fine(fine(invs[0][b], grad, 1, 0), invs[1][b], 1, 0)

    def precondition_down(b):
        grad = jnp.concatenate([sum_of(("D", b, 0, c)) for c in range(4)], axis=1)
        res[1][b] = fine(invs[3][b], fine(grad, invs[2][b], 1, 1), 0, 0).T

    tick(1, 3)
    tick(0, 7)
    tick(2, 1)
    tick(1, 4)
    tick(0, 8)
    tick(2, 2)
    tick(1, 5)
    symmetric("H", 2, 0)
    tick(1, 6)
    tick(2, 3)
    symmetric("H", 2, 1)
    tick(2, 4)
    tick(1, 7)
    narrow("A", 0, 0)
    narrow("Q", 3, 1)
    tick(2, 5)
    tick(1, 8)
    precondition_down(1)
    tick(2, 6)
    symmetric("S", 1, 1)
    tick(2, 7)
    narrow("A", 0, 1)
    narrow("Q", 3, 0)
    precondition_up(1)
    precondition_down(0)
    tick(2, 8)
    symmetric("S", 1, 0)
    precondition_up(0)
    stores = [pltpu.make_async_copy(src, dst, out_sem.at[n]) for n, (src, dst) in enumerate(zip(tuple(res) + tuple(new), outs))]
    for store in stores:
        store.start()
    for piece in range(len(PIECES)):
        for stage in range(4):
            halving(piece, stage).wait_send()
            doubling(piece, stage).wait_send()
    for store in stores:
        store.wait()


def solution(mesh):
    axis_size = mesh.shape["data"]

    def local_step(tokens, out_grad, w_up, w_down, a_up_old, s_up_old, a_down_old, s_down_old,
                   a_up_inv, s_up_inv, a_down_inv, s_down_inv, factor_decay):
        rows = tokens.shape[0]
        count = rows // (2 * TILE)
        small, wide = (2, 128, 128), (2, 512, 512)
        out_shapes = ((2, 128, 512), (2, 512, 128), small, wide, wide, small)

        def kernel(tok, og, wu, wd, rho, *refs):
            body(axis_size, rows, tok, og, wu, wd, rho, refs[0:4], refs[4:8], refs[8:14],
                 *refs[14:21], refs[21:23], *refs[23:32], refs[32:36], refs[36:40], refs[40:42], *refs[42:])

        anywhere = pl.BlockSpec(memory_space=pl.ANY)
        inside = pl.BlockSpec(memory_space=pltpu.VMEM)
        half = lambda *shape: pltpu.VMEM(shape, BF)
        full = lambda *shape: pltpu.VMEM(shape, F32)
        sems = pltpu.SemaphoreType.DMA
        return tuple(pl.pallas_call(
            kernel,
            in_specs=[anywhere] * 2 + [inside] * 2 + [pl.BlockSpec(memory_space=pltpu.SMEM)] + [anywhere] * 8,
            out_specs=[anywhere] * 6,
            out_shape=[jax.ShapeDtypeStruct(s, F32) for s in out_shapes],
            scratch_shapes=[half(rows, 128), half(rows, 128), half(512, rows), half(512, rows), half(512, rows), half(128, rows),
                            half(128, rows), half(1280, TILE), half(1280, TILE), half(2, 512, 128), half(128, 512),
                            full(2, 640, 256), full(2, 384, 256), full(256, 256), full(128, 512),
                            full(TOTAL_ROWS, 128), full(TOTAL_ROWS - TOTAL_ROWS // 16, 128), full(TOTAL_ROWS, 128)]
            + [full(*s) for s in out_shapes[2:]] * 2 + [full(*s) for s in out_shapes[:2]]
            + [sems((2 * count + 8,)), sems((6,)), sems((2, 4, len(PIECES))), sems((2, 4, len(PIECES)))],
            compiler_params=pltpu.CompilerParams(vmem_limit_bytes=63 * 2**20, collective_id=0, has_side_effects=True),
        )(tokens, out_grad, w_up, w_down, factor_decay.reshape(1), a_up_old, s_up_old, a_down_old, s_down_old,
          a_up_inv, s_up_inv, a_down_inv, s_down_inv))

    batch_spec = P("data", None)
    return jax.shard_map(local_step, mesh=mesh, in_specs=(batch_spec, batch_spec) + (P(),) * 11,
                         out_specs=(P(),) * 6, check_vma=False)
```

```python
import jax
import jax.numpy as jnp
from jax import lax
from jax.experimental import pallas as pl
from jax.experimental.pallas import tpu as pltpu
from jax.sharding import PartitionSpec as P

BF = jnp.bfloat16
F32 = jnp.float32
MESH = pl.DeviceIdType.MESH
HIGH = lax.Precision.HIGHEST
C0 = 0.7978845608028654
CA = C0 * 0.044715
TILE = 512
CHUNK = 512
STRIDE = {"c": 1, "x": 2, "y": 4, "z": 8}
ORDERS = ("cxyz", "cyzx", "czxy")

LOWER = [(r, c) for c in range(4) for r in range(c, 4)]
MIXED = [(0, 0), (1, 0), (1, 1), (2, 2), (3, 2), (3, 3), (0, 2), (1, 2), (0, 3), (1, 3)]
KEPT = {("S", 0): LOWER, ("S", 1): LOWER, ("H", 0): LOWER, ("H", 1): MIXED}


def tri(kind, b):
    return [(kind, b, r, c) for r, c in KEPT[(kind, b)]]


def row(kind, b):
    return [(kind, b, 0, c) for c in range(4)]


GROUPS = (
    (6, row("D", 1) + [("A", 0, 0, 0), ("Q", 1, 0, 0)] + tri("H", 0) + tri("H", 1)),
    (6, row("U", 1) + row("D", 0) + [("A", 1, 0, 0), ("Q", 0, 0, 0)] + tri("S", 1)),
    (6, row("U", 0) + tri("S", 0)),
)
PLAN1 = ((1, 0, 1), (6, 0, 2), (10, 0, 3), (14, 0, 4))
PLAN2 = ((2, 0, 5), (2, 1, 1), (5, 0, 6), (9, 1, 2))
SLOT = {}
PIECES = []
GROUP_PIECES = []
for _count, _blocks in GROUPS:
    _members = []
    for _n in range(_count):
        _size = -(-len(_blocks) // (_count - _n))
        _members.append(len(PIECES))
        PIECES.append((ORDERS[_n % 3], 128 * len(SLOT), 128 * _size))
        for _block in _blocks[:_size]:
            SLOT[_block] = 128 * len(SLOT)
        _blocks = _blocks[_size:]
    GROUP_PIECES.append(_members)
TOTAL_ROWS = 128 * len(SLOT)


def mm(a, b):
    return lax.dot_general(a, b, (((1,), (0,)), ((), ())), preferred_element_type=F32)


def nt(a, b):
    return lax.dot_general(a, b, (((1,), (1,)), ((), ())), preferred_element_type=F32)


def fine(a, b, ca, cb):
    return lax.dot_general(a, b, (((ca,), (cb,)), ((), ())), precision=HIGH, preferred_element_type=F32)


def rounded(x):
    return x.astype(BF).astype(F32)


def gelu_parts(z):
    sq = z * z
    cub = CA * sq
    base = cub + C0
    th = jnp.tanh(z * base)
    return cub, base, th, 0.5 * th + 0.5


def gelu(z):
    return z * gelu_parts(z)[3]


def gelu_slope(z):
    cub, base, th, half = gelu_parts(z)
    return half + (z * half) * ((base + (cub + cub)) * (1.0 - th))


def weave(first, second):
    done = 0
    for n, step in enumerate(first):
        step()
        while done < len(second) and (done + 1) * len(first) <= (n + 1) * len(second):
            second[done]()
            done += 1
    for step in second[done:]:
        step()


def body(axis_size, rows, tok_hbm, og_hbm, wu, wd, rho, old_hbm, inv_hbm, res, new,
         tok, og, pre0, pre1, hid0, mid, grad0, tiles, wut, wdt, acc_a, acc_b, acc_c, acc_d, part, recv, total, invs,
         load_sem, send_sem, recv_sem):
    me = lax.axis_index("data")
    bit = {d: (me // s) % 2 for d, s in STRIDE.items()}
    count = rows // (2 * TILE)
    scale = 1.0 / (axis_size * rows)

    def tok_load(n):
        here = pl.ds(pl.multiple_of(n * (2 * TILE), 2 * TILE), 2 * TILE)
        return pltpu.make_async_copy(tok_hbm.at[here, :], tok.at[here, :], load_sem.at[n])

    def og_load(n):
        here = pl.ds(pl.multiple_of(n * (2 * TILE), 2 * TILE), 2 * TILE)
        return pltpu.make_async_copy(og_hbm.at[here, :], og.at[here, :], load_sem.at[count + n])

    late_loads = [pltpu.make_async_copy(src, dst, load_sem.at[2 * count + n])
                  for n, (src, dst) in enumerate(zip(tuple(old_hbm) + tuple(inv_hbm), tuple(new) + tuple(invs)))]

    def spot(piece, stage):
        order, base, size = PIECES[piece]
        at = base
        for s in range(stage):
            at = at + bit[order[s]] * (size >> (s + 1))
        return at

    def share(piece, hop, gather):
        order, base, size = PIECES[piece]
        part_size = size >> (hop + 1) if hop < 2 else size >> 4
        found = []
        for way in range(1, 2 if hop < 2 else 4):
            if hop < 2:
                kept, dims = hop + 1, order[hop]
            else:
                kept, dims = 4, (order[2:3] if way == 1 else order[3:4] if way == 2 else order[2:4])
            at = spot(piece, kept)
            target = me
            away = at
            for d in dims:
                target = target + STRIDE[d] - 2 * STRIDE[d] * bit[d]
                length = size >> (order.index(d) + 1)
                away = away + length - 2 * length * bit[d]
            lane = hop + way - 1
            if gather:
                here = pl.ds(pl.multiple_of(at, 8), part_size)
                src, dst = total.at[here, :], total.at[here, :]
            else:
                src = part.at[pl.ds(pl.multiple_of(away, 8), part_size), :]
                dst = recv.at[pl.ds(inbox(piece, hop) + (way - 1) * part_size, part_size), :]
            found.append(pltpu.make_async_remote_copy(
                src_ref=src, dst_ref=dst, send_sem=send_sem.at[gather, lane, piece], recv_sem=recv_sem.at[gather, lane, piece],
                device_id=(target,), device_id_type=MESH))
        return found

    def inbox(piece, hop):
        _, base, size = PIECES[piece]
        return base - base // 16 + (0, size // 2, size // 2 + size // 4)[hop]

    def start(copies):
        for copy in copies:
            copy.start()

    def arrive(copies):
        for copy in copies:
            copy.wait_recv()

    def tick(group, step, pieces=None):
        for piece in GROUP_PIECES[group] if pieces is None else pieces:
            order, _, size = PIECES[piece]
            if step == 0:
                start(share(piece, 0, 0))
            elif step == 1:
                arrive(share(piece, 0, 0))
                at, box, half = spot(piece, 1), inbox(piece, 0), size >> 2
                keep = bit[order[1]] * half
                for shift in (half - keep, keep):
                    here = pl.ds(pl.multiple_of(at + shift, 8), half)
                    there = pl.ds(pl.multiple_of(box + shift, 8), half)
                    part[here, :] = part[here, :] + recv[there, :]
                start(share(piece, 1, 0))
            elif step == 2:
                arrive(share(piece, 1, 0))
                here = pl.ds(pl.multiple_of(spot(piece, 2), 8), size >> 2)
                box = inbox(piece, 1)
                part[here, :] = part[here, :] + recv[box:box + (size >> 2), :]
                start(share(piece, 2, 0))
            elif step == 3:
                arrive(share(piece, 2, 0))
                here = pl.ds(pl.multiple_of(spot(piece, 4), 8), size >> 4)
                box, q = inbox(piece, 2), size >> 4
                total[here, :] = (part[here, :] + recv[box:box + q, :]) + (recv[box + q:box + 2 * q, :] + recv[box + 2 * q:box + 3 * q, :])
                start(share(piece, 2, 1))
            else:
                arrive(share(piece, 6 - step, 1))
                if step < 6:
                    start(share(piece, 5 - step, 1))

    def near(n):
        return pl.ds(pl.multiple_of(n * TILE, TILE), TILE)

    def chunks(make):
        return [make(f) for f in range(0, 512, CHUNK)]

    def acts0(tile, n):
        kept = {}

        def start():
            kept["u"] = tok[near(n), :].T
            tile[512:640, :] = kept["u"]
            tile[640:768, :] = og[near(n), :].T

        def first(f):
            def step():
                pre = mm(wut[0, f:f + CHUNK, :], kept["u"]).astype(BF)
                pre0[f:f + CHUNK, near(n)] = pre
                hid = gelu(pre.astype(F32)).astype(BF)
                tile[f:f + CHUNK, :] = hid
                hid0[f:f + CHUNK, near(n)] = hid
            return step

        def middle():
            kept["m"] = mm(wdt[...], tile[0:512, :]).astype(BF)
            mid[:, near(n)] = kept["m"]

        def second(f):
            def step():
                pre = mm(wut[1, f:f + CHUNK, :], kept["m"]).astype(BF)
                pre1[f:f + CHUNK, near(n)] = pre
                tile[768 + f:768 + f + CHUNK, :] = gelu(pre.astype(F32)).astype(BF)
            return step

        return [start] + chunks(first) + [middle] + chunks(second)

    def left_sums(tile, k, size):
        def one():
            acc_a[k, 0:size, :] += nt(tile[0:size, :], tile[0:256, :])

        def two():
            acc_b[k, 0:size - 256, :] += nt(tile[256:size, :], tile[256:512, :])

        return [one, two]

    def narrow_sums(tile):
        def one():
            acc_c[...] += nt(tile[512:768, :], tile[512:768, :])

        return [one]

    def sums0(tile, n):
        def one():
            acc_a[1] += nt(tile[640:1280, :], tile[1024:1280, :])

        def two():
            acc_b[1] += nt(tile[640:1024, :], tile[768:1024, :])

        return left_sums(tile, 0, 512) + narrow_sums(tile) + [one, two]

    def acts1(tile, n):
        kept = {}

        def start():
            kept["q"] = og[near(n), :].T
            tile[512:640, :] = mid[:, near(n)]

        def chunk(f):
            def step():
                back = rounded(mm(wd[1, f:f + CHUNK, :], kept["q"]))
                tile[f:f + CHUNK, :] = (back * gelu_slope(pre1[f:f + CHUNK, near(n)].astype(F32))).astype(BF)
            return step

        def end():
            grad = mm(wu[1], tile[0:512, :]).astype(BF)
            tile[640:768, :] = grad
            grad0[:, near(n)] = grad

        return [start] + chunks(chunk) + [end]

    def sums1(tile, n):
        def one():
            acc_d[...] += nt(tile[640:768, :], hid0[:, near(n)])

        return left_sums(tile, 0, 640) + narrow_sums(tile) + [one]

    def acts2(tile, n):
        def start():
            tile[512:640, :] = tok[near(n), :].T

        def chunk(f):
            def step():
                back = rounded(mm(wd[0, f:f + CHUNK, :], grad0[:, near(n)]))
                tile[f:f + CHUNK, :] = (back * gelu_slope(pre0[f:f + CHUNK, near(n)].astype(F32))).astype(BF)
            return step

        return [start] + chunks(chunk)

    def sums2(tile, n):
        return left_sums(tile, 0, 640)

    def phase(acts, sums, ticks):
        for acc in (acc_a, acc_b, acc_c, acc_d):
            acc[...] = jnp.zeros_like(acc)
        tiles[1][...] = jnp.zeros_like(tiles[1])

        def step(j, _):
            if acts is acts0:
                tok_load(j).wait()
                og_load(j).wait()
            for side in range(2):
                n = 2 * j + side
                weave(acts(tiles[side], n), sums(tiles[1 - side], (n + 2 * count - 1) % (2 * count)))
                for when, group, what in ticks:
                    if when % 2 == side:
                        @pl.when(j == when // 2)
                        def _():
                            tick(group, what)
            return 0

        lax.fori_loop(0, count, step, 0)
        for last in sums(tiles[1], 2 * count - 1):
            last()

    def put(block, value):
        part[SLOT[block]:SLOT[block] + 128, :] = value * scale

    def block_of(r, c):
        return slice(128 * r, 128 * r + 128), slice(128 * c, 128 * c + 128)

    def put_left(kind, b):
        for r, c in LOWER:
            rows_at, cols_at = block_of(r - 2 * (c > 1), c % 2)
            put((kind, b, r, c), (acc_b if c > 1 else acc_a)[0, rows_at, cols_at])
        if kind == "S":
            for c in range(4):
                rows_at, cols_at = block_of(4 - 2 * (c > 1), c % 2)
                put(("U", b, 0, c), (acc_b if c > 1 else acc_a)[0, rows_at, cols_at])

    def put_right(b):
        for r, c in MIXED:
            rows_at, cols_at = block_of(r + 1, c % 2)
            put(("H", b, r, c), (acc_a if c > 1 else acc_b)[1, rows_at, cols_at])
        for c in range(4):
            rows_at, cols_at = block_of(0, c % 2)
            put(("D", b, 0, c), (acc_a if c > 1 else acc_b)[1, rows_at, cols_at])

    barrier = pltpu.get_barrier_semaphore()
    for dims in ("c", "x", "y", "z", "xy", "yz", "zx"):
        target = me
        for d in dims:
            target = target + STRIDE[d] - 2 * STRIDE[d] * bit[d]
        pl.semaphore_signal(barrier, inc=1, device_id=(target,), device_id_type=MESH)
    for n in range(count):
        tok_load(n).start()
        og_load(n).start()
    wut[0] = wu[0].T
    wut[1] = wu[1].T
    wdt[...] = wd[0].T

    phase(acts0, sums0, ())
    for load in late_loads:
        load.start()
    put_left("H", 0)
    put_right(1)
    put(("A", 0, 0, 0), acc_c[0:128, 0:128])
    put(("Q", 1, 0, 0), acc_c[128:256, 128:256])
    pl.semaphore_wait(barrier, 7)
    tick(0, 0)

    phase(acts1, sums1, PLAN1)
    put_left("S", 1)
    put(("A", 1, 0, 0), acc_c[0:128, 0:128])
    put(("Q", 0, 0, 0), acc_c[128:256, 128:256])
    for c in range(4):
        put(("D", 0, 0, c), acc_d[:, 128 * c:128 * c + 128])
    tick(1, 0)

    phase(acts2, sums2, PLAN2)
    put_left("S", 0)
    tick(2, 0)

    keep = rho[0]
    fresh = 1.0 - keep

    for load in late_loads:
        load.wait()

    def sum_of(block):
        return total[SLOT[block]:SLOT[block] + 128, :]

    def blend(n, b, r, c, value):
        rows_at, cols_at = block_of(r, c)
        new[n][b, rows_at, cols_at] = keep * new[n][b, rows_at, cols_at] + fresh * value

    def symmetric(kind, n, b):
        for r, c in KEPT[(kind, b)]:
            value = sum_of((kind, b, r, c))
            blend(n, b, r, c, value)
            if r != c:
                blend(n, b, c, r, value.T)

    def narrow(kind, n, b):
        blend(n, b, 0, 0, sum_of((kind, b, 0, 0)))

    def precondition_up(b):
        grad = jnp.concatenate([sum_of(("U", b, 0, c)) for c in range(4)], axis=1)
        res[0][b] = fine(fine(invs[0][b], grad, 1, 0), invs[1][b], 1, 0)

    def precondition_down(b):
        grad = jnp.concatenate([sum_of(("D", b, 0, c)) for c in range(4)], axis=1)
        res[1][b] = fine(invs[3][b], fine(grad, invs[2][b], 1, 1), 0, 0).T

    tick(2, 1)
    tick(1, 3)
    tick(2, 2)
    symmetric("H", 2, 0)
    tick(1, 4)
    tick(2, 3)
    symmetric("H", 2, 1)
    tick(1, 5)
    narrow("A", 0, 0)
    narrow("Q", 3, 1)
    tick(2, 4)
    tick(1, 6)
    precondition_down(1)
    symmetric("S", 1, 1)
    tick(2, 5)
    narrow("A", 0, 1)
    narrow("Q", 3, 0)
    precondition_up(1)
    precondition_down(0)
    tick(2, 6)
    symmetric("S", 1, 0)
    precondition_up(0)
    for piece in range(len(PIECES)):
        for hop in range(3):
            for copy in share(piece, hop, 0) + share(piece, hop, 1):
                copy.wait_send()


def solution(mesh):
    axis_size = mesh.shape["data"]

    def local_step(tokens, out_grad, w_up, w_down, a_up_old, s_up_old, a_down_old, s_down_old,
                   a_up_inv, s_up_inv, a_down_inv, s_down_inv, factor_decay):
        rows = tokens.shape[0]
        count = rows // (2 * TILE)
        small, wide = (2, 128, 128), (2, 512, 512)
        out_shapes = ((2, 128, 512), (2, 512, 128), small, wide, wide, small)

        def kernel(tok, og, wu, wd, rho, *refs):
            body(axis_size, rows, tok, og, wu, wd, rho, refs[0:4], refs[4:8], refs[8:10], refs[10:14],
                 *refs[14:21], refs[21:23], *refs[23:32], refs[32:36], *refs[36:])

        anywhere = pl.BlockSpec(memory_space=pl.ANY)
        inside = pl.BlockSpec(memory_space=pltpu.VMEM)
        half = lambda *shape: pltpu.VMEM(shape, BF)
        full = lambda *shape: pltpu.VMEM(shape, F32)
        sems = pltpu.SemaphoreType.DMA
        found = pl.pallas_call(
            kernel,
            in_specs=[anywhere] * 2 + [inside] * 2 + [pl.BlockSpec(memory_space=pltpu.SMEM)] + [anywhere] * 8,
            out_specs=[inside] * 6,
            out_shape=[full(*s) for s in out_shapes],
            scratch_shapes=[half(rows, 128), half(rows, 128), half(512, rows), half(512, rows), half(512, rows), half(128, rows),
                            half(128, rows), half(1280, TILE), half(1280, TILE), half(2, 512, 128), half(128, 512),
                            full(2, 640, 256), full(2, 384, 256), full(256, 256), full(128, 512),
                            full(TOTAL_ROWS, 128), full(TOTAL_ROWS - TOTAL_ROWS // 16, 128), full(TOTAL_ROWS, 128)]
            + [full(*s) for s in out_shapes[2:]]
            + [sems((2 * count + 8,)), sems((2, 5, len(PIECES))), sems((2, 5, len(PIECES)))],
            compiler_params=pltpu.CompilerParams(vmem_limit_bytes=57 * 2**20, collective_id=0, has_side_effects=True),
        )(tokens, out_grad, w_up, w_down, factor_decay.reshape(1), a_up_old, s_up_old, a_down_old, s_down_old,
          a_up_inv, s_up_inv, a_down_inv, s_down_inv)

        def put_out(*refs):
            stores = [pltpu.make_async_copy(refs[n], refs[6 + n], refs[12].at[n]) for n in range(6)]
            for store in stores:
                store.start()
            for store in stores:
                store.wait()

        return tuple(pl.pallas_call(
            put_out,
            in_specs=[inside] * 6,
            out_specs=[anywhere] * 6,
            out_shape=[jax.ShapeDtypeStruct(s, F32) for s in out_shapes],
            scratch_shapes=[sems((6,))],
            compiler_params=pltpu.CompilerParams(vmem_limit_bytes=2**20),
        )(*[pltpu.with_memory_space_constraint(x, pltpu.VMEM) for x in found]))

    batch_spec = P("data", None)
    return jax.shard_map(local_step, mesh=mesh, in_specs=(batch_spec, batch_spec) + (P(),) * 11,
                         out_specs=(P(),) * 6, check_vma=False)
```

```python
import jax
import jax.numpy as jnp
from jax import lax
from jax.experimental import pallas as pl
from jax.experimental.pallas import tpu as pltpu
from jax.sharding import PartitionSpec as P

BF = jnp.bfloat16
F32 = jnp.float32
MESH = pl.DeviceIdType.MESH
HIGH = lax.Precision.HIGHEST
C0 = 0.7978845608028654
CA = C0 * 0.044715
TILE = 512
CHUNK = 512
STRIDE = {"c": 1, "x": 2, "y": 4, "z": 8}
ORDERS = ("cxyz", "cyzx", "czxy")

LOWER = [(r, c) for c in range(4) for r in range(c, 4)]
MIXED = [(0, 0), (1, 0), (1, 1), (2, 2), (3, 2), (3, 3), (0, 2), (1, 2), (0, 3), (1, 3)]
KEPT = {("S", 0): LOWER, ("S", 1): LOWER, ("H", 0): LOWER, ("H", 1): MIXED}


def tri(kind, b):
    return [(kind, b, r, c) for r, c in KEPT[(kind, b)]]


def row(kind, b):
    return [(kind, b, 0, c) for c in range(4)]


GROUPS = (
    (6, row("D", 1) + [("A", 0, 0, 0), ("Q", 1, 0, 0)] + tri("H", 0) + tri("H", 1)),
    (6, row("U", 1) + row("D", 0) + [("A", 1, 0, 0), ("Q", 0, 0, 0)] + tri("S", 1)),
    (6, row("U", 0) + tri("S", 0)),
)
PLAN1 = ((1, 0, 1), (7, 0, 2), (11, 0, 3), (15, 0, 4))
PLAN2 = ((3, 0, 5), (4, 1, 1), (6, 0, 6), (11, 1, 2), (15, 1, 3))
SLOT = {}
PIECES = []
GROUP_PIECES = []
for _count, _blocks in GROUPS:
    _members = []
    for _n in range(_count):
        _size = -(-len(_blocks) // (_count - _n))
        _members.append(len(PIECES))
        PIECES.append((ORDERS[_n % 3], 128 * len(SLOT), 128 * _size))
        for _block in _blocks[:_size]:
            SLOT[_block] = 128 * len(SLOT)
        _blocks = _blocks[_size:]
    GROUP_PIECES.append(_members)
TOTAL_ROWS = 128 * len(SLOT)


def mm(a, b):
    return lax.dot_general(a, b, (((1,), (0,)), ((), ())), preferred_element_type=F32)


def nt(a, b):
    return lax.dot_general(a, b, (((1,), (1,)), ((), ())), preferred_element_type=F32)


def fine(a, b, ca, cb):
    return lax.dot_general(a, b, (((ca,), (cb,)), ((), ())), precision=HIGH, preferred_element_type=F32)


def rounded(x):
    return x.astype(BF).astype(F32)


def gelu_parts(z):
    sq = z * z
    cub = CA * sq
    base = cub + C0
    th = jnp.tanh(z * base)
    return cub, base, th, 0.5 * th + 0.5


def gelu(z):
    return z * gelu_parts(z)[3]


def gelu_slope(z):
    cub, base, th, half = gelu_parts(z)
    return half + (z * half) * ((base + (cub + cub)) * (1.0 - th))


def weave(first, second):
    done = 0
    for n, step in enumerate(first):
        step()
        while done < len(second) and (done + 1) * len(first) <= (n + 1) * len(second):
            second[done]()
            done += 1
    for step in second[done:]:
        step()


def body(axis_size, rows, tok_hbm, og_hbm, wu_hbm, wd_hbm, rho, old_hbm, inv_hbm, res, new,
         tok, og, wu, wd, pre0, pre1, hid0, mid, grad0, tiles, wut, wdt, acc_a, acc_b, acc_c, acc_d, part, recv, total, invs,
         load_sem, send_sem, recv_sem):
    me = lax.axis_index("data")
    bit = {d: (me // s) % 2 for d, s in STRIDE.items()}
    count = rows // (2 * TILE)
    scale = 1.0 / (axis_size * rows)

    def tok_load(n):
        here = pl.ds(pl.multiple_of(n * (2 * TILE), 2 * TILE), 2 * TILE)
        return pltpu.make_async_copy(tok_hbm.at[here, :], tok.at[here, :], load_sem.at[n])

    def og_load(n):
        here = pl.ds(pl.multiple_of(n * (2 * TILE), 2 * TILE), 2 * TILE)
        return pltpu.make_async_copy(og_hbm.at[here, :], og.at[here, :], load_sem.at[count + n])

    wu_load = pltpu.make_async_copy(wu_hbm, wu, load_sem.at[2 * count + 8])
    wd_load = pltpu.make_async_copy(wd_hbm, wd, load_sem.at[2 * count + 9])
    late_loads = [pltpu.make_async_copy(src, dst, load_sem.at[2 * count + n])
                  for n, (src, dst) in enumerate(zip(tuple(old_hbm) + tuple(inv_hbm), tuple(new) + tuple(invs)))]

    def spot(piece, stage):
        order, base, size = PIECES[piece]
        at = base
        for s in range(stage):
            at = at + bit[order[s]] * (size >> (s + 1))
        return at

    def share(piece, hop, gather):
        order, base, size = PIECES[piece]
        part_size = size >> (hop + 1) if hop < 2 else size >> 4
        found = []
        for way in range(1, 2 if hop < 2 else 4):
            if hop < 2:
                kept, dims = hop + 1, order[hop]
            else:
                kept, dims = 4, (order[2:3] if way == 1 else order[3:4] if way == 2 else order[2:4])
            at = spot(piece, kept)
            target = me
            away = at
            for d in dims:
                target = target + STRIDE[d] - 2 * STRIDE[d] * bit[d]
                length = size >> (order.index(d) + 1)
                away = away + length - 2 * length * bit[d]
            lane = hop + way - 1
            if gather:
                here = pl.ds(pl.multiple_of(at, 8), part_size)
                src, dst = total.at[here, :], total.at[here, :]
            else:
                src = part.at[pl.ds(pl.multiple_of(away, 8), part_size), :]
                dst = recv.at[pl.ds(inbox(piece, hop) + (way - 1) * part_size, part_size), :]
            found.append(pltpu.make_async_remote_copy(
                src_ref=src, dst_ref=dst, send_sem=send_sem.at[gather, lane, piece], recv_sem=recv_sem.at[gather, lane, piece],
                device_id=(target,), device_id_type=MESH))
        return found

    def inbox(piece, hop):
        _, base, size = PIECES[piece]
        return base - base // 16 + (0, size // 2, size // 2 + size // 4)[hop]

    def start(copies):
        for copy in copies:
            copy.start()

    def arrive(copies):
        for copy in copies:
            copy.wait_recv()

    def tick(group, step, pieces=None):
        for piece in GROUP_PIECES[group] if pieces is None else pieces:
            order, _, size = PIECES[piece]
            if step == 0:
                start(share(piece, 0, 0))
            elif step == 1:
                arrive(share(piece, 0, 0))
                at, box, half = spot(piece, 1), inbox(piece, 0), size >> 2
                keep = bit[order[1]] * half
                for shift in (half - keep, keep):
                    here = pl.ds(pl.multiple_of(at + shift, 8), half)
                    there = pl.ds(pl.multiple_of(box + shift, 8), half)
                    part[here, :] = part[here, :] + recv[there, :]
                start(share(piece, 1, 0))
            elif step == 2:
                arrive(share(piece, 1, 0))
                here = pl.ds(pl.multiple_of(spot(piece, 2), 8), size >> 2)
                box = inbox(piece, 1)
                part[here, :] = part[here, :] + recv[box:box + (size >> 2), :]
                start(share(piece, 2, 0))
            elif step == 3:
                arrive(share(piece, 2, 0))
                here = pl.ds(pl.multiple_of(spot(piece, 4), 8), size >> 4)
                box, q = inbox(piece, 2), size >> 4
                total[here, :] = (part[here, :] + recv[box:box + q, :]) + (recv[box + q:box + 2 * q, :] + recv[box + 2 * q:box + 3 * q, :])
                start(share(piece, 2, 1))
            else:
                arrive(share(piece, 6 - step, 1))
                if step < 6:
                    start(share(piece, 5 - step, 1))

    def near(n):
        return pl.ds(pl.multiple_of(n * TILE, TILE), TILE)

    def chunks(make):
        return [make(f) for f in range(0, 512, CHUNK)]

    def acts0(tile, n):
        kept = {}

        def start():
            kept["u"] = tok[near(n), :].T
            tile[512:640, :] = kept["u"]
            tile[640:768, :] = og[near(n), :].T

        def first(f):
            def step():
                pre = mm(wut[0, f:f + CHUNK, :], kept["u"]).astype(BF)
                pre0[f:f + CHUNK, near(n)] = pre
                hid = gelu(pre.astype(F32)).astype(BF)
                tile[f:f + CHUNK, :] = hid
                hid0[f:f + CHUNK, near(n)] = hid
            return step

        def middle():
            kept["m"] = mm(wdt[...], tile[0:512, :]).astype(BF)
            mid[:, near(n)] = kept["m"]

        def second(f):
            def step():
                pre = mm(wut[1, f:f + CHUNK, :], kept["m"]).astype(BF)
                pre1[f:f + CHUNK, near(n)] = pre
                tile[768 + f:768 + f + CHUNK, :] = gelu(pre.astype(F32)).astype(BF)
            return step

        return [start] + chunks(first) + [middle] + chunks(second)

    def left_sums(tile, k, size):
        def one():
            acc_a[k, 0:size, :] += nt(tile[0:size, :], tile[0:256, :])

        def two():
            acc_b[k, 0:size - 256, :] += nt(tile[256:size, :], tile[256:512, :])

        return [one, two]

    def narrow_sums(tile):
        def one():
            acc_c[...] += nt(tile[512:768, :], tile[512:768, :])

        return [one]

    def sums0(tile, n):
        def one():
            acc_a[1] += nt(tile[640:1280, :], tile[1024:1280, :])

        def two():
            acc_b[1] += nt(tile[640:1024, :], tile[768:1024, :])

        return [one, two] + left_sums(tile, 0, 512) + narrow_sums(tile)

    def acts1(tile, n):
        kept = {}

        def start():
            kept["q"] = og[near(n), :].T
            tile[512:640, :] = mid[:, near(n)]

        def chunk(f):
            def step():
                back = rounded(mm(wd[1, f:f + CHUNK, :], kept["q"]))
                tile[f:f + CHUNK, :] = (back * gelu_slope(pre1[f:f + CHUNK, near(n)].astype(F32))).astype(BF)
            return step

        def end():
            grad = mm(wu[1], tile[0:512, :]).astype(BF)
            tile[640:768, :] = grad
            grad0[:, near(n)] = grad

        return [start] + chunks(chunk) + [end]

    def sums1(tile, n):
        def one():
            acc_d[...] += nt(tile[640:768, :], hid0[:, near(n)])

        return left_sums(tile, 0, 640) + narrow_sums(tile) + [one]

    def acts2(tile, n):
        def start():
            tile[512:640, :] = tok[near(n), :].T

        def chunk(f):
            def step():
                back = rounded(mm(wd[0, f:f + CHUNK, :], grad0[:, near(n)]))
                tile[f:f + CHUNK, :] = (back * gelu_slope(pre0[f:f + CHUNK, near(n)].astype(F32))).astype(BF)
            return step

        return [start] + chunks(chunk)

    def sums2(tile, n):
        return left_sums(tile, 0, 640)

    def phase(acts, sums, ticks):
        for acc in (acc_a, acc_b, acc_c, acc_d):
            acc[...] = jnp.zeros_like(acc)
        tiles[1][...] = jnp.zeros_like(tiles[1])

        def step(j, _):
            if acts is acts0:
                tok_load(j).wait()
                og_load(j).wait()
            for side in range(2):
                n = 2 * j + side
                weave(acts(tiles[side], n), sums(tiles[1 - side], (n + 2 * count - 1) % (2 * count)))
                for when, group, what in ticks:
                    if when % 2 == side:
                        @pl.when(j == when // 2)
                        def _():
                            tick(group, what)
            return 0

        lax.fori_loop(0, count, step, 0)
        for last in sums(tiles[1], 2 * count - 1):
            last()

    def put(block, value):
        part[SLOT[block]:SLOT[block] + 128, :] = value * scale

    def block_of(r, c):
        return slice(128 * r, 128 * r + 128), slice(128 * c, 128 * c + 128)

    def put_left(kind, b):
        for r, c in LOWER:
            rows_at, cols_at = block_of(r - 2 * (c > 1), c % 2)
            put((kind, b, r, c), (acc_b if c > 1 else acc_a)[0, rows_at, cols_at])
        if kind == "S":
            for c in range(4):
                rows_at, cols_at = block_of(4 - 2 * (c > 1), c % 2)
                put(("U", b, 0, c), (acc_b if c > 1 else acc_a)[0, rows_at, cols_at])

    def put_right(b):
        for r, c in MIXED:
            rows_at, cols_at = block_of(r + 1, c % 2)
            put(("H", b, r, c), (acc_a if c > 1 else acc_b)[1, rows_at, cols_at])
        for c in range(4):
            rows_at, cols_at = block_of(0, c % 2)
            put(("D", b, 0, c), (acc_a if c > 1 else acc_b)[1, rows_at, cols_at])

    tok_load(0).start()
    wu_load.start()
    wd_load.start()
    og_load(0).start()
    for n in range(1, count):
        tok_load(n).start()
        og_load(n).start()
    barrier = pltpu.get_barrier_semaphore()
    for dims in ("c", "x", "y", "z", "xy", "yz", "zx"):
        target = me
        for d in dims:
            target = target + STRIDE[d] - 2 * STRIDE[d] * bit[d]
        pl.semaphore_signal(barrier, inc=1, device_id=(target,), device_id_type=MESH)
    wu_load.wait()
    wd_load.wait()
    wut[0] = wu[0].T
    wut[1] = wu[1].T
    wdt[...] = wd[0].T

    phase(acts0, sums0, ())
    for load in late_loads:
        load.start()
    put_left("H", 0)
    put_right(1)
    put(("A", 0, 0, 0), acc_c[0:128, 0:128])
    put(("Q", 1, 0, 0), acc_c[128:256, 128:256])
    pl.semaphore_wait(barrier, 7)
    tick(0, 0)

    phase(acts1, sums1, PLAN1)
    put_left("S", 1)
    put(("A", 1, 0, 0), acc_c[0:128, 0:128])
    put(("Q", 0, 0, 0), acc_c[128:256, 128:256])
    for c in range(4):
        put(("D", 0, 0, c), acc_d[:, 128 * c:128 * c + 128])
    tick(1, 0)

    phase(acts2, sums2, PLAN2)
    put_left("S", 0)
    tick(2, 0)

    keep = rho[0]
    fresh = 1.0 - keep

    for load in late_loads:
        load.wait()

    def sum_of(block):
        return total[SLOT[block]:SLOT[block] + 128, :]

    def blend(n, b, r, c, value):
        rows_at, cols_at = block_of(r, c)
        new[n][b, rows_at, cols_at] = keep * new[n][b, rows_at, cols_at] + fresh * value

    def symmetric(kind, n, b):
        for r, c in KEPT[(kind, b)]:
            value = sum_of((kind, b, r, c))
            blend(n, b, r, c, value)
            if r != c:
                blend(n, b, c, r, value.T)

    def narrow(kind, n, b):
        blend(n, b, 0, 0, sum_of((kind, b, 0, 0)))

    def precondition_up(b):
        grad = jnp.concatenate([sum_of(("U", b, 0, c)) for c in range(4)], axis=1)
        res[0][b] = fine(fine(invs[0][b], grad, 1, 0), invs[1][b], 1, 0)

    def precondition_down(b):
        grad = jnp.concatenate([sum_of(("D", b, 0, c)) for c in range(4)], axis=1)
        res[1][b] = fine(invs[3][b], fine(grad, invs[2][b], 1, 1), 0, 0).T

    tick(2, 1)
    symmetric("H", 2, 0)
    tick(2, 2)
    tick(1, 4)
    tick(2, 3)
    symmetric("H", 2, 1)
    tick(1, 5)
    narrow("A", 0, 0)
    narrow("Q", 3, 1)
    tick(2, 4)
    tick(1, 6)
    precondition_down(1)
    symmetric("S", 1, 1)
    tick(2, 5)
    narrow("A", 0, 1)
    narrow("Q", 3, 0)
    precondition_up(1)
    precondition_down(0)
    tick(2, 6)
    symmetric("S", 1, 0)
    precondition_up(0)
    for piece in range(len(PIECES)):
        for hop in range(3):
            for copy in share(piece, hop, 0) + share(piece, hop, 1):
                copy.wait_send()


def solution(mesh):
    axis_size = mesh.shape["data"]

    def local_step(tokens, out_grad, w_up, w_down, a_up_old, s_up_old, a_down_old, s_down_old,
                   a_up_inv, s_up_inv, a_down_inv, s_down_inv, factor_decay):
        rows = tokens.shape[0]
        count = rows // (2 * TILE)
        small, wide = (2, 128, 128), (2, 512, 512)
        out_shapes = ((2, 128, 512), (2, 512, 128), small, wide, wide, small)

        def kernel(tok, og, wu, wd, rho, *refs):
            body(axis_size, rows, tok, og, wu, wd, rho, refs[0:4], refs[4:8], refs[8:10], refs[10:14],
                 *refs[14:23], refs[23:25], *refs[25:34], refs[34:38], *refs[38:])

        anywhere = pl.BlockSpec(memory_space=pl.ANY)
        inside = pl.BlockSpec(memory_space=pltpu.VMEM)
        half = lambda *shape: pltpu.VMEM(shape, BF)
        full = lambda *shape: pltpu.VMEM(shape, F32)
        sems = pltpu.SemaphoreType.DMA
        found = pl.pallas_call(
            kernel,
            in_specs=[anywhere] * 4 + [pl.BlockSpec(memory_space=pltpu.SMEM)] + [anywhere] * 8,
            out_specs=[inside] * 6,
            out_shape=[full(*s) for s in out_shapes],
            scratch_shapes=[half(rows, 128), half(rows, 128), half(2, 128, 512), half(2, 512, 128), half(512, rows), half(512, rows), half(512, rows), half(128, rows),
                            half(128, rows), half(1280, TILE), half(1280, TILE), half(2, 512, 128), half(128, 512),
                            full(2, 640, 256), full(2, 384, 256), full(256, 256), full(128, 512),
                            full(TOTAL_ROWS, 128), full(TOTAL_ROWS - TOTAL_ROWS // 16, 128), full(TOTAL_ROWS, 128)]
            + [full(*s) for s in out_shapes[2:]]
            + [sems((2 * count + 10,)), sems((2, 5, len(PIECES))), sems((2, 5, len(PIECES)))],
            compiler_params=pltpu.CompilerParams(vmem_limit_bytes=57 * 2**20, collective_id=0, has_side_effects=True),
        )(tokens, out_grad, w_up, w_down, factor_decay.reshape(1), a_up_old, s_up_old, a_down_old, s_down_old,
          a_up_inv, s_up_inv, a_down_inv, s_down_inv)

        def put_out(*refs):
            stores = [pltpu.make_async_copy(refs[n], refs[6 + n], refs[12].at[n]) for n in range(6)]
            for store in stores:
                store.start()
            for store in stores:
                store.wait()

        return tuple(pl.pallas_call(
            put_out,
            in_specs=[inside] * 6,
            out_specs=[anywhere] * 6,
            out_shape=[jax.ShapeDtypeStruct(s, F32) for s in out_shapes],
            scratch_shapes=[sems((6,))],
            compiler_params=pltpu.CompilerParams(vmem_limit_bytes=2**20),
        )(*[pltpu.with_memory_space_constraint(x, pltpu.VMEM) for x in found]))

    batch_spec = P("data", None)
    return jax.shard_map(local_step, mesh=mesh, in_specs=(batch_spec, batch_spec) + (P(),) * 11,
                         out_specs=(P(),) * 6, check_vma=False)
```

```python
import jax
import jax.numpy as jnp
from jax import lax
from jax.experimental import pallas as pl
from jax.experimental.pallas import tpu as pltpu
from jax.sharding import PartitionSpec as P

BF = jnp.bfloat16
F32 = jnp.float32
MESH = pl.DeviceIdType.MESH
HIGH = lax.Precision.HIGHEST
C0 = 0.7978845608028654
CA = C0 * 0.044715
LANES = 128
WIDE = 512
TILE = 512
CHUNK = WIDE
STRIDE = {"c": 1, "x": 2, "y": 4, "z": 8}
ORDERS = ("cxyz", "cyzx", "czxy")

LOWER = [(r, c) for c in range(4) for r in range(c, 4)]
MIXED = [(0, 0), (1, 0), (1, 1), (2, 2), (3, 2), (3, 3), (0, 2), (1, 2), (0, 3), (1, 3)]
KEPT = {("S", 0): LOWER, ("S", 1): LOWER, ("H", 0): LOWER, ("H", 1): MIXED}


def tri(kind, b):
    return [(kind, b, r, c) for r, c in KEPT[(kind, b)]]


def row(kind, b):
    return [(kind, b, 0, c) for c in range(4)]


GROUPS = (
    (3, row("D", 1) + [("A", 0, 0, 0), ("Q", 1, 0, 0)] + tri("H", 0) + tri("H", 1)),
    (3, row("U", 1) + row("D", 0) + [("A", 1, 0, 0), ("Q", 0, 0, 0)] + tri("S", 1)),
    (6, row("U", 0) + tri("S", 0)),
)
PLAN1 = ((1, 0, 1), (7, 0, 2), (11, 0, 3), (15, 0, 4))
PLAN2 = ((3, 0, 5), (4, 1, 1), (6, 0, 6), (11, 1, 2), (15, 1, 3))
SLOT = {}
PIECES = []
GROUP_PIECES = []
for _count, _blocks in GROUPS:
    _members = []
    for _n in range(_count):
        _size = -(-len(_blocks) // (_count - _n))
        _members.append(len(PIECES))
        PIECES.append((ORDERS[_n % 3], LANES * len(SLOT), LANES * _size))
        for _block in _blocks[:_size]:
            SLOT[_block] = LANES * len(SLOT)
        _blocks = _blocks[_size:]
    GROUP_PIECES.append(_members)
TOTAL_ROWS = LANES * len(SLOT)


def mm(a, b):
    return lax.dot_general(a, b, (((1,), (0,)), ((), ())), preferred_element_type=F32)


def nt(a, b):
    return lax.dot_general(a, b, (((1,), (1,)), ((), ())), preferred_element_type=F32)


def fine(a, b, ca, cb):
    return lax.dot_general(a, b, (((ca,), (cb,)), ((), ())), precision=HIGH, preferred_element_type=F32)


def rounded(x):
    return x.astype(BF).astype(F32)


def gelu_parts(z):
    sq = z * z
    cub = CA * sq
    base = cub + C0
    th = jnp.tanh(z * base)
    return cub, base, th, 0.5 * th + 0.5


def gelu(z):
    return z * gelu_parts(z)[3]


def gelu_slope(z):
    cub, base, th, half = gelu_parts(z)
    return half + (z * half) * ((base + (cub + cub)) * (1.0 - th))


def weave(first, second):
    done = 0
    for n, step in enumerate(first):
        step()
        while done < len(second) and (done + 1) * len(first) <= (n + 1) * len(second):
            second[done]()
            done += 1
    for step in second[done:]:
        step()


def body(axis_size, rows, tok_hbm, og_hbm, wu_hbm, wd_hbm, rho, old_hbm, inv_hbm, res, new,
         tok, og, wu, wd, pre0, pre1, hid0, mid, grad0, tiles, wut, wdt, acc_a, acc_b, acc_c, acc_d, part, recv, total, invs,
         load_sem, send_sem, recv_sem):
    me = lax.axis_index("data")
    bit = {d: (me // s) % 2 for d, s in STRIDE.items()}
    count = rows // (2 * TILE)
    scale = 1.0 / (axis_size * rows)

    def tok_load(n):
        here = pl.ds(pl.multiple_of(n * (2 * TILE), 2 * TILE), 2 * TILE)
        return pltpu.make_async_copy(tok_hbm.at[here, :], tok.at[here, :], load_sem.at[n])

    def og_load(n):
        here = pl.ds(pl.multiple_of(n * (2 * TILE), 2 * TILE), 2 * TILE)
        return pltpu.make_async_copy(og_hbm.at[here, :], og.at[here, :], load_sem.at[count + n])

    wu_load = pltpu.make_async_copy(wu_hbm, wu, load_sem.at[2 * count + 8])
    wd_load = pltpu.make_async_copy(wd_hbm, wd, load_sem.at[2 * count + 9])
    late_loads = [pltpu.make_async_copy(src, dst, load_sem.at[2 * count + n])
                  for n, (src, dst) in enumerate(zip(tuple(old_hbm) + tuple(inv_hbm), tuple(new) + tuple(invs)))]

    def spot(piece, stage):
        order, base, size = PIECES[piece]
        at = base
        for s in range(stage):
            at = at + bit[order[s]] * (size >> (s + 1))
        return at

    def share(piece, hop, gather):
        order, base, size = PIECES[piece]
        part_size = size >> (hop + 1) if hop < 2 else size >> 4
        found = []
        for way in range(1, 2 if hop < 2 else 4):
            if hop < 2:
                kept, dims = hop + 1, order[hop]
            else:
                kept, dims = 4, (order[2:3] if way == 1 else order[3:4] if way == 2 else order[2:4])
            at = spot(piece, kept)
            target = me
            away = at
            for d in dims:
                target = target + STRIDE[d] - 2 * STRIDE[d] * bit[d]
                length = size >> (order.index(d) + 1)
                away = away + length - 2 * length * bit[d]
            lane = hop + way - 1
            if gather:
                here = pl.ds(pl.multiple_of(at, 8), part_size)
                src, dst = total.at[here, :], total.at[here, :]
            else:
                src = part.at[pl.ds(pl.multiple_of(away, 8), part_size), :]
                dst = recv.at[pl.ds(inbox(piece, hop) + (way - 1) * part_size, part_size), :]
            found.append(pltpu.make_async_remote_copy(
                src_ref=src, dst_ref=dst, send_sem=send_sem.at[gather, lane, piece], recv_sem=recv_sem.at[gather, lane, piece],
                device_id=(target,), device_id_type=MESH))
        return found

    def inbox(piece, hop):
        _, base, size = PIECES[piece]
        return base - base // 16 + (0, size // 2, size // 2 + size // 4)[hop]

    def start(copies):
        for copy in copies:
            copy.start()

    def arrive(copies):
        for copy in copies:
            copy.wait_recv()

    def tick(group, step, pieces=None):
        for piece in GROUP_PIECES[group] if pieces is None else pieces:
            order, _, size = PIECES[piece]
            if step == 0:
                start(share(piece, 0, 0))
            elif step == 1:
                arrive(share(piece, 0, 0))
                at, box, half = spot(piece, 1), inbox(piece, 0), size >> 2
                keep = bit[order[1]] * half
                for shift in (half - keep, keep):
                    here = pl.ds(pl.multiple_of(at + shift, 8), half)
                    there = pl.ds(pl.multiple_of(box + shift, 8), half)
                    part[here, :] = part[here, :] + recv[there, :]
                start(share(piece, 1, 0))
            elif step == 2:
                arrive(share(piece, 1, 0))
                here = pl.ds(pl.multiple_of(spot(piece, 2), 8), size >> 2)
                box = inbox(piece, 1)
                part[here, :] = part[here, :] + recv[box:box + (size >> 2), :]
                start(share(piece, 2, 0))
            elif step == 3:
                arrive(share(piece, 2, 0))
                here = pl.ds(pl.multiple_of(spot(piece, 4), 8), size >> 4)
                box, q = inbox(piece, 2), size >> 4
                total[here, :] = (part[here, :] + recv[box:box + q, :]) + (recv[box + q:box + 2 * q, :] + recv[box + 2 * q:box + 3 * q, :])
                start(share(piece, 2, 1))
            else:
                arrive(share(piece, 6 - step, 1))
                if step < 6:
                    start(share(piece, 5 - step, 1))

    def near(n):
        return pl.ds(pl.multiple_of(n * TILE, TILE), TILE)

    def chunks(make):
        return [make(f) for f in range(0, WIDE, CHUNK)]

    def acts0(tile, n):
        kept = {}

        def start():
            kept["u"] = tok[near(n), :].T
            tile[WIDE:640, :] = kept["u"]
            tile[640:768, :] = og[near(n), :].T

        def first(f):
            def step():
                pre = mm(wut[0, f:f + CHUNK, :], kept["u"]).astype(BF)
                pre0[f:f + CHUNK, near(n)] = pre
                hid = gelu(pre.astype(F32)).astype(BF)
                tile[f:f + CHUNK, :] = hid
                hid0[f:f + CHUNK, near(n)] = hid
            return step

        def middle():
            kept["m"] = mm(wdt[...], tile[0:WIDE, :]).astype(BF)
            mid[:, near(n)] = kept["m"]

        def second(f):
            def step():
                pre = mm(wut[1, f:f + CHUNK, :], kept["m"]).astype(BF)
                pre1[f:f + CHUNK, near(n)] = pre
                tile[768 + f:768 + f + CHUNK, :] = gelu(pre.astype(F32)).astype(BF)
            return step

        return [start] + chunks(first) + [middle] + chunks(second)

    def left_sums(tile, k, size):
        def one():
            acc_a[k, 0:size, :] += nt(tile[0:size, :], tile[0:256, :])

        def two():
            acc_b[k, 0:size - 256, :] += nt(tile[256:size, :], tile[256:WIDE, :])

        return [one, two]

    def narrow_sums(tile):
        def one():
            acc_c[...] += nt(tile[WIDE:768, :], tile[WIDE:768, :])

        return [one]

    def sums0(tile, n):
        def one():
            acc_a[1] += nt(tile[640:1280, :], tile[1024:1280, :])

        def two():
            acc_b[1] += nt(tile[640:1024, :], tile[768:1024, :])

        return [one, two] + left_sums(tile, 0, WIDE) + narrow_sums(tile)

    def acts1(tile, n):
        kept = {}

        def start():
            kept["q"] = og[near(n), :].T
            tile[WIDE:640, :] = mid[:, near(n)]

        def chunk(f):
            def step():
                back = rounded(mm(wd[1, f:f + CHUNK, :], kept["q"]))
                tile[f:f + CHUNK, :] = (back * gelu_slope(pre1[f:f + CHUNK, near(n)].astype(F32))).astype(BF)
            return step

        def end():
            grad = mm(wu[1], tile[0:WIDE, :]).astype(BF)
            tile[640:768, :] = grad
            grad0[:, near(n)] = grad

        return [start] + chunks(chunk) + [end]

    def sums1(tile, n):
        def one():
            acc_d[...] += nt(tile[640:768, :], hid0[:, near(n)])

        return left_sums(tile, 0, 640) + narrow_sums(tile) + [one]

    def acts2(tile, n):
        def start():
            tile[WIDE:640, :] = tok[near(n), :].T

        def chunk(f):
            def step():
                back = rounded(mm(wd[0, f:f + CHUNK, :], grad0[:, near(n)]))
                tile[f:f + CHUNK, :] = (back * gelu_slope(pre0[f:f + CHUNK, near(n)].astype(F32))).astype(BF)
            return step

        return [start] + chunks(chunk)

    def sums2(tile, n):
        return left_sums(tile, 0, 640)

    def phase(acts, sums, ticks):
        for acc in (acc_a, acc_b, acc_c, acc_d):
            acc[...] = jnp.zeros_like(acc)
        tiles[1][...] = jnp.zeros_like(tiles[1])

        def step(j, _):
            if acts is acts0:
                tok_load(j).wait()
                og_load(j).wait()
            for side in range(2):
                n = 2 * j + side
                weave(acts(tiles[side], n), sums(tiles[1 - side], (n + 2 * count - 1) % (2 * count)))
                for when, group, what in ticks:
                    if when % 2 == side:
                        @pl.when(j == when // 2)
                        def _():
                            tick(group, what)
            return 0

        lax.fori_loop(0, count, step, 0)
        for last in sums(tiles[1], 2 * count - 1):
            last()

    def put(block, value):
        part[SLOT[block]:SLOT[block] + LANES, :] = value * scale

    def block_of(r, c):
        return slice(LANES * r, LANES * r + LANES), slice(LANES * c, LANES * c + LANES)

    def put_left(kind, b):
        for r, c in LOWER:
            rows_at, cols_at = block_of(r - 2 * (c > 1), c % 2)
            put((kind, b, r, c), (acc_b if c > 1 else acc_a)[0, rows_at, cols_at])
        if kind == "S":
            for c in range(4):
                rows_at, cols_at = block_of(4 - 2 * (c > 1), c % 2)
                put(("U", b, 0, c), (acc_b if c > 1 else acc_a)[0, rows_at, cols_at])

    def put_right(b):
        for r, c in MIXED:
            rows_at, cols_at = block_of(r + 1, c % 2)
            put(("H", b, r, c), (acc_a if c > 1 else acc_b)[1, rows_at, cols_at])
        for c in range(4):
            rows_at, cols_at = block_of(0, c % 2)
            put(("D", b, 0, c), (acc_a if c > 1 else acc_b)[1, rows_at, cols_at])

    tok_load(0).start()
    wu_load.start()
    wd_load.start()
    og_load(0).start()
    for n in range(1, count):
        tok_load(n).start()
        og_load(n).start()
    barrier = pltpu.get_barrier_semaphore()
    for dims in ("c", "x", "y", "z", "xy", "yz", "zx"):
        target = me
        for d in dims:
            target = target + STRIDE[d] - 2 * STRIDE[d] * bit[d]
        pl.semaphore_signal(barrier, inc=1, device_id=(target,), device_id_type=MESH)
    wu_load.wait()
    wd_load.wait()
    wut[0] = wu[0].T
    wut[1] = wu[1].T
    wdt[...] = wd[0].T

    phase(acts0, sums0, ())
    for load in late_loads:
        load.start()
    put_left("H", 0)
    put_right(1)
    put(("A", 0, 0, 0), acc_c[0:LANES, 0:LANES])
    put(("Q", 1, 0, 0), acc_c[LANES:256, LANES:256])
    pl.semaphore_wait(barrier, 7)
    tick(0, 0)

    phase(acts1, sums1, PLAN1)
    put_left("S", 1)
    put(("A", 1, 0, 0), acc_c[0:LANES, 0:LANES])
    put(("Q", 0, 0, 0), acc_c[LANES:256, LANES:256])
    for c in range(4):
        put(("D", 0, 0, c), acc_d[:, LANES * c:LANES * c + LANES])
    tick(1, 0)

    phase(acts2, sums2, PLAN2)
    put_left("S", 0)
    tick(2, 0)

    keep = rho[0]
    fresh = 1.0 - keep

    for load in late_loads:
        load.wait()

    def sum_of(block):
        return total[SLOT[block]:SLOT[block] + LANES, :]

    def blend(n, b, r, c, value):
        rows_at, cols_at = block_of(r, c)
        new[n][b, rows_at, cols_at] = keep * new[n][b, rows_at, cols_at] + fresh * value

    def symmetric(kind, n, b):
        for r, c in KEPT[(kind, b)]:
            value = sum_of((kind, b, r, c))
            blend(n, b, r, c, value)
            if r != c:
                blend(n, b, c, r, value.T)

    def narrow(kind, n, b):
        blend(n, b, 0, 0, sum_of((kind, b, 0, 0)))

    def precondition_up(b):
        grad = jnp.concatenate([sum_of(("U", b, 0, c)) for c in range(4)], axis=1)
        res[0][b] = fine(fine(invs[0][b], grad, 1, 0), invs[1][b], 1, 0)

    def precondition_down(b):
        grad = jnp.concatenate([sum_of(("D", b, 0, c)) for c in range(4)], axis=1)
        res[1][b] = fine(invs[3][b], fine(grad, invs[2][b], 1, 1), 0, 0).T

    tick(2, 1)
    symmetric("H", 2, 0)
    tick(2, 2)
    tick(1, 4)
    tick(2, 3)
    symmetric("H", 2, 1)
    tick(1, 5)
    narrow("A", 0, 0)
    narrow("Q", 3, 1)
    tick(2, 4)
    tick(1, 6)
    precondition_down(1)
    symmetric("S", 1, 1)
    tick(2, 5)
    narrow("A", 0, 1)
    narrow("Q", 3, 0)
    precondition_up(1)
    precondition_down(0)
    tick(2, 6)
    symmetric("S", 1, 0)
    precondition_up(0)
    for piece in range(len(PIECES)):
        for hop in range(3):
            for copy in share(piece, hop, 0) + share(piece, hop, 1):
                copy.wait_send()


def solution(mesh):
    axis_size = mesh.shape["data"]

    def local_step(tokens, out_grad, w_up, w_down, a_up_old, s_up_old, a_down_old, s_down_old,
                   a_up_inv, s_up_inv, a_down_inv, s_down_inv, factor_decay):
        rows = tokens.shape[0]
        count = rows // (2 * TILE)
        small, wide = (2, LANES, LANES), (2, WIDE, WIDE)
        out_shapes = ((2, LANES, WIDE), (2, WIDE, LANES), small, wide, wide, small)

        def kernel(tok, og, wu, wd, rho, *refs):
            body(axis_size, rows, tok, og, wu, wd, rho, refs[0:4], refs[4:8], refs[8:10], refs[10:14],
                 *refs[14:23], refs[23:25], *refs[25:34], refs[34:38], *refs[38:])

        anywhere = pl.BlockSpec(memory_space=pl.ANY)
        inside = pl.BlockSpec(memory_space=pltpu.VMEM)
        half = lambda *shape: pltpu.VMEM(shape, BF)
        full = lambda *shape: pltpu.VMEM(shape, F32)
        sems = pltpu.SemaphoreType.DMA
        found = pl.pallas_call(
            kernel,
            in_specs=[anywhere] * 4 + [pl.BlockSpec(memory_space=pltpu.SMEM)] + [anywhere] * 8,
            out_specs=[inside] * 6,
            out_shape=[full(*s) for s in out_shapes],
            scratch_shapes=[half(rows, LANES), half(rows, LANES), half(2, LANES, WIDE), half(2, WIDE, LANES), half(WIDE, rows), half(WIDE, rows), half(WIDE, rows), half(LANES, rows),
                            half(LANES, rows), half(1280, TILE), half(1280, TILE), half(2, WIDE, LANES), half(LANES, WIDE),
                            full(2, 640, 256), full(2, 384, 256), full(256, 256), full(LANES, WIDE),
                            full(TOTAL_ROWS, LANES), full(TOTAL_ROWS - TOTAL_ROWS // 16, LANES), full(TOTAL_ROWS, LANES)]
            + [full(*s) for s in out_shapes[2:]]
            + [sems((2 * count + 10,)), sems((2, 5, len(PIECES))), sems((2, 5, len(PIECES)))],
            compiler_params=pltpu.CompilerParams(vmem_limit_bytes=57 * 2**20, collective_id=0, has_side_effects=True),
        )(tokens, out_grad, w_up, w_down, factor_decay.reshape(1), a_up_old, s_up_old, a_down_old, s_down_old,
          a_up_inv, s_up_inv, a_down_inv, s_down_inv)

        def put_out(*refs):
            stores = [pltpu.make_async_copy(refs[n], refs[6 + n], refs[12].at[n]) for n in range(6)]
            for store in stores:
                store.start()
            for store in stores:
                store.wait()

        return tuple(pl.pallas_call(
            put_out,
            in_specs=[inside] * 6,
            out_specs=[anywhere] * 6,
            out_shape=[jax.ShapeDtypeStruct(s, F32) for s in out_shapes],
            scratch_shapes=[sems((6,))],
            compiler_params=pltpu.CompilerParams(vmem_limit_bytes=2**20),
        )(*[pltpu.with_memory_space_constraint(x, pltpu.VMEM) for x in found]))

    batch_spec = P("data", None)
    return jax.shard_map(local_step, mesh=mesh, in_specs=(batch_spec, batch_spec) + (P(),) * 11,
                         out_specs=(P(),) * 6, check_vma=False)
```

```python
import jax
import jax.numpy as jnp
from jax import lax
from jax.experimental import pallas as pl
from jax.experimental.pallas import tpu as pltpu
from jax.sharding import PartitionSpec as P

BF = jnp.bfloat16
F32 = jnp.float32
MESH = pl.DeviceIdType.MESH
HIGH = lax.Precision.HIGHEST
C0 = 0.7978845608028654
CA = C0 * 0.044715
LANES = 128
WIDE = 512
TILE = 512
CHUNK = WIDE
STRIDE = {"c": 1, "x": 2, "y": 4, "z": 8}
ORDERS = ("cxyz", "cyzx", "czxy")

LOWER = [(r, c) for c in range(4) for r in range(c, 4)]
MIXED = [(0, 0), (1, 0), (1, 1), (2, 2), (3, 2), (3, 3), (0, 2), (1, 2), (0, 3), (1, 3)]
KEPT = {("S", 0): LOWER, ("S", 1): LOWER, ("H", 0): LOWER, ("H", 1): MIXED}


def tri(kind, b):
    return [(kind, b, r, c) for r, c in KEPT[(kind, b)]]


def row(kind, b):
    return [(kind, b, 0, c) for c in range(4)]


GROUPS = (
    (3, row("D", 1) + [("A", 0, 0, 0), ("Q", 1, 0, 0)] + tri("H", 0) + tri("H", 1)),
    (3, row("U", 1) + row("D", 0) + [("A", 1, 0, 0), ("Q", 0, 0, 0)] + tri("S", 1)),
    (6, row("U", 0) + tri("S", 0)),
)
PLAN1 = ((1, 0, 1), (7, 0, 2), (11, 0, 3), (15, 0, 4))
PLAN2 = ((3, 0, 5), (4, 1, 1), (6, 0, 6), (11, 1, 2), (15, 1, 3))
SLOT = {}
PIECES = []
GROUP_PIECES = []
for _count, _blocks in GROUPS:
    _members = []
    for _n in range(_count):
        _size = -(-len(_blocks) // (_count - _n))
        _members.append(len(PIECES))
        PIECES.append((ORDERS[_n % 3], LANES * len(SLOT), LANES * _size))
        for _block in _blocks[:_size]:
            SLOT[_block] = LANES * len(SLOT)
        _blocks = _blocks[_size:]
    GROUP_PIECES.append(_members)
TOTAL_ROWS = LANES * len(SLOT)


def mm(a, b):
    return lax.dot_general(a, b, (((1,), (0,)), ((), ())), preferred_element_type=F32)


def nt(a, b):
    return lax.dot_general(a, b, (((1,), (1,)), ((), ())), preferred_element_type=F32)


def fine(a, b, ca, cb):
    return lax.dot_general(a, b, (((ca,), (cb,)), ((), ())), precision=HIGH, preferred_element_type=F32)


def rounded(x):
    return x.astype(BF).astype(F32)


def gelu_parts(z):
    sq = z * z
    cub = CA * sq
    base = cub + C0
    th = jnp.tanh(z * base)
    return cub, base, th, 0.5 * th + 0.5


def gelu(z):
    return z * gelu_parts(z)[3]


def gelu_slope(z):
    cub, base, th, half = gelu_parts(z)
    return half + (z * half) * ((base + (cub + cub)) * (1.0 - th))


def weave(first, second):
    done = 0
    for n, step in enumerate(first):
        step()
        while done < len(second) and (done + 1) * len(first) <= (n + 1) * len(second):
            second[done]()
            done += 1
    for step in second[done:]:
        step()


def body(axis_size, rows, tok_hbm, og_hbm, wu_hbm, wd_hbm, rho, old_hbm, inv_hbm, res, new,
         tok, og, wu, wd, pre0, pre1, hid0, mid, grad0, tiles, wut, wdt, acc_a, acc_b, acc_c, acc_d, part, recv, total, invs,
         load_sem, send_sem, recv_sem):
    me = lax.axis_index("data")
    bit = {d: (me // s) % 2 for d, s in STRIDE.items()}
    count = rows // (2 * TILE)
    scale = 1.0 / (axis_size * rows)

    def tok_load(n):
        here = pl.ds(pl.multiple_of(n * (2 * TILE), 2 * TILE), 2 * TILE)
        return pltpu.make_async_copy(tok_hbm.at[here, :], tok.at[here, :], load_sem.at[n])

    def og_load(n):
        here = pl.ds(pl.multiple_of(n * (2 * TILE), 2 * TILE), 2 * TILE)
        return pltpu.make_async_copy(og_hbm.at[here, :], og.at[here, :], load_sem.at[count + n])

    wu_load = pltpu.make_async_copy(wu_hbm, wu, load_sem.at[2 * count + 8])
    wd_load = pltpu.make_async_copy(wd_hbm, wd, load_sem.at[2 * count + 9])
    late_loads = [pltpu.make_async_copy(src, dst, load_sem.at[2 * count + n])
                  for n, (src, dst) in enumerate(zip(tuple(old_hbm) + tuple(inv_hbm), tuple(new) + tuple(invs)))]

    def spot(piece, stage):
        order, base, size = PIECES[piece]
        at = base
        for s in range(stage):
            at = at + bit[order[s]] * (size >> (s + 1))
        return at

    def share(piece, hop, gather):
        order, base, size = PIECES[piece]
        part_size = size >> (hop + 1) if hop < 2 else size >> 4
        found = []
        for way in range(1, 2 if hop < 2 else 4):
            if hop < 2:
                kept, dims = hop + 1, order[hop]
            else:
                kept, dims = 4, (order[2:3] if way == 1 else order[3:4] if way == 2 else order[2:4])
            at = spot(piece, kept)
            target = me
            away = at
            for d in dims:
                target = target + STRIDE[d] - 2 * STRIDE[d] * bit[d]
                length = size >> (order.index(d) + 1)
                away = away + length - 2 * length * bit[d]
            lane = hop + way - 1
            if gather:
                here = pl.ds(pl.multiple_of(at, 8), part_size)
                src, dst = total.at[here, :], total.at[here, :]
            else:
                src = part.at[pl.ds(pl.multiple_of(away, 8), part_size), :]
                dst = recv.at[pl.ds(inbox(piece, hop) + (way - 1) * part_size, part_size), :]
            found.append(pltpu.make_async_remote_copy(
                src_ref=src, dst_ref=dst, send_sem=send_sem.at[gather, lane, piece], recv_sem=recv_sem.at[gather, lane, piece],
                device_id=(target,), device_id_type=MESH))
        return found

    def inbox(piece, hop):
        _, base, size = PIECES[piece]
        return base - base // 16 + (0, size // 2, size // 2 + size // 4)[hop]

    def start(copies):
        for copy in copies:
            copy.start()

    def arrive(copies):
        for copy in copies:
            copy.wait_recv()

    def tick(group, step, pieces=None):
        for piece in GROUP_PIECES[group] if pieces is None else pieces:
            order, _, size = PIECES[piece]
            if step == 0:
                start(share(piece, 0, 0))
            elif step == 1:
                arrive(share(piece, 0, 0))
                at, box, half = spot(piece, 1), inbox(piece, 0), size >> 2
                keep = bit[order[1]] * half
                for shift in (half - keep, keep):
                    here = pl.ds(pl.multiple_of(at + shift, 8), half)
                    there = pl.ds(pl.multiple_of(box + shift, 8), half)
                    part[here, :] = part[here, :] + recv[there, :]
                start(share(piece, 1, 0))
            elif step == 2:
                arrive(share(piece, 1, 0))
                here = pl.ds(pl.multiple_of(spot(piece, 2), 8), size >> 2)
                box = inbox(piece, 1)
                part[here, :] = part[here, :] + recv[box:box + (size >> 2), :]
                start(share(piece, 2, 0))
            elif step == 3:
                arrive(share(piece, 2, 0))
                here = pl.ds(pl.multiple_of(spot(piece, 4), 8), size >> 4)
                box, q = inbox(piece, 2), size >> 4
                total[here, :] = (part[here, :] + recv[box:box + q, :]) + (recv[box + q:box + 2 * q, :] + recv[box + 2 * q:box + 3 * q, :])
                start(share(piece, 2, 1))
            else:
                arrive(share(piece, 6 - step, 1))
                if step < 6:
                    start(share(piece, 5 - step, 1))

    def near(n):
        return pl.ds(pl.multiple_of(n * TILE, TILE), TILE)

    def chunks(make):
        return [make(f) for f in range(0, WIDE, CHUNK)]

    def acts0(tile, n):
        kept = {}

        def start():
            kept["u"] = tok[near(n), :].T
            tile[WIDE:640, :] = kept["u"]
            tile[640:768, :] = og[near(n), :].T

        def first(f):
            def step():
                pre = mm(wut[0, f:f + CHUNK, :], kept["u"]).astype(BF)
                pre0[f:f + CHUNK, near(n)] = pre
                hid = gelu(pre.astype(F32)).astype(BF)
                tile[f:f + CHUNK, :] = hid
                hid0[f:f + CHUNK, near(n)] = hid
            return step

        def middle():
            kept["m"] = mm(wdt[...], tile[0:WIDE, :]).astype(BF)
            mid[:, near(n)] = kept["m"]

        def second(f):
            def step():
                pre = mm(wut[1, f:f + CHUNK, :], kept["m"]).astype(BF)
                pre1[f:f + CHUNK, near(n)] = pre
                tile[768 + f:768 + f + CHUNK, :] = gelu(pre.astype(F32)).astype(BF)
            return step

        return [start] + chunks(first) + [middle] + chunks(second)

    def left_sums(tile, k, size):
        def one():
            acc_a[k, 0:size, :] += nt(tile[0:size, :], tile[0:256, :])

        def two():
            acc_b[k, 0:size - 256, :] += nt(tile[256:size, :], tile[256:WIDE, :])

        return [one, two]

    def narrow_sums(tile):
        def one():
            acc_c[...] += nt(tile[WIDE:768, :], tile[WIDE:768, :])

        return [one]

    def sums0(tile, n):
        def one():
            acc_a[1] += nt(tile[640:1280, :], tile[1024:1280, :])

        def two():
            acc_b[1] += nt(tile[640:1024, :], tile[768:1024, :])

        return [one, two] + left_sums(tile, 0, WIDE) + narrow_sums(tile)

    def acts1(tile, n):
        kept = {}

        def start():
            kept["q"] = og[near(n), :].T
            tile[WIDE:640, :] = mid[:, near(n)]

        def chunk(f):
            def step():
                back = rounded(mm(wd[1, f:f + CHUNK, :], kept["q"]))
                tile[f:f + CHUNK, :] = (back * gelu_slope(pre1[f:f + CHUNK, near(n)].astype(F32))).astype(BF)
            return step

        def end():
            grad = mm(wu[1], tile[0:WIDE, :]).astype(BF)
            tile[640:768, :] = grad
            grad0[:, near(n)] = grad

        return [start] + chunks(chunk) + [end]

    def sums1(tile, n):
        def one():
            acc_d[...] += nt(tile[640:768, :], hid0[:, near(n)])

        return left_sums(tile, 0, 640) + narrow_sums(tile) + [one]

    def acts2(tile, n):
        def start():
            tile[WIDE:640, :] = tok[near(n), :].T

        def chunk(f):
            def step():
                back = rounded(mm(wd[0, f:f + CHUNK, :], grad0[:, near(n)]))
                tile[f:f + CHUNK, :] = (back * gelu_slope(pre0[f:f + CHUNK, near(n)].astype(F32))).astype(BF)
            return step

        return [start] + chunks(chunk)

    def sums2(tile, n):
        return left_sums(tile, 0, 640)

    def phase(acts, sums, ticks):
        for acc in (acc_a, acc_b, acc_c, acc_d):
            acc[...] = jnp.zeros_like(acc)
        tiles[1][...] = jnp.zeros_like(tiles[1])

        def step(j, _):
            if acts is acts0:
                tok_load(j).wait()
                og_load(j).wait()
            for side in range(2):
                n = 2 * j + side
                weave(acts(tiles[side], n), sums(tiles[1 - side], (n + 2 * count - 1) % (2 * count)))
                for when, group, what in ticks:
                    if when % 2 == side:
                        @pl.when(j == when // 2)
                        def _():
                            tick(group, what)
            return 0

        lax.fori_loop(0, count, step, 0)
        for last in sums(tiles[1], 2 * count - 1):
            last()

    def put(block, value):
        part[SLOT[block]:SLOT[block] + LANES, :] = value * scale

    def block_of(r, c):
        return slice(LANES * r, LANES * r + LANES), slice(LANES * c, LANES * c + LANES)

    def put_left(kind, b):
        for r, c in LOWER:
            rows_at, cols_at = block_of(r - 2 * (c > 1), c % 2)
            put((kind, b, r, c), (acc_b if c > 1 else acc_a)[0, rows_at, cols_at])
        if kind == "S":
            for c in range(4):
                rows_at, cols_at = block_of(4 - 2 * (c > 1), c % 2)
                put(("U", b, 0, c), (acc_b if c > 1 else acc_a)[0, rows_at, cols_at])

    def put_right(b):
        for r, c in MIXED:
            rows_at, cols_at = block_of(r + 1, c % 2)
            put(("H", b, r, c), (acc_a if c > 1 else acc_b)[1, rows_at, cols_at])
        for c in range(4):
            rows_at, cols_at = block_of(0, c % 2)
            put(("D", b, 0, c), (acc_a if c > 1 else acc_b)[1, rows_at, cols_at])

    tok_load(0).start()
    wu_load.start()
    wd_load.start()
    og_load(0).start()
    for n in range(1, count):
        tok_load(n).start()
        og_load(n).start()
    barrier = pltpu.get_barrier_semaphore()
    for dims in ("c", "x", "y", "z", "xy", "yz", "zx"):
        target = me
        for d in dims:
            target = target + STRIDE[d] - 2 * STRIDE[d] * bit[d]
        pl.semaphore_signal(barrier, inc=1, device_id=(target,), device_id_type=MESH)
    wu_load.wait()
    wd_load.wait()
    wut[0] = wu[0].T
    wut[1] = wu[1].T
    wdt[...] = wd[0].T

    phase(acts0, sums0, ())
    for load in late_loads:
        load.start()
    put_left("H", 0)
    put_right(1)
    put(("A", 0, 0, 0), acc_c[0:LANES, 0:LANES])
    put(("Q", 1, 0, 0), acc_c[LANES:256, LANES:256])
    pl.semaphore_wait(barrier, 7)
    tick(0, 0)

    phase(acts1, sums1, PLAN1)
    put_left("S", 1)
    put(("A", 1, 0, 0), acc_c[0:LANES, 0:LANES])
    put(("Q", 0, 0, 0), acc_c[LANES:256, LANES:256])
    for c in range(4):
        put(("D", 0, 0, c), acc_d[:, LANES * c:LANES * c + LANES])
    tick(1, 0)

    phase(acts2, sums2, PLAN2)
    put_left("S", 0)
    tick(2, 0)

    keep = rho[0]
    fresh = 1.0 - keep

    for load in late_loads:
        load.wait()

    def sum_of(block):
        return total[SLOT[block]:SLOT[block] + LANES, :]

    def blend(n, b, r, c, value):
        rows_at, cols_at = block_of(r, c)
        new[n][b, rows_at, cols_at] = keep * new[n][b, rows_at, cols_at] + fresh * value

    def symmetric(kind, n, b):
        for r, c in KEPT[(kind, b)]:
            value = sum_of((kind, b, r, c))
            blend(n, b, r, c, value)
            if r != c:
                blend(n, b, c, r, value.T)

    def narrow(kind, n, b):
        blend(n, b, 0, 0, sum_of((kind, b, 0, 0)))

    def precondition_up(b):
        grad = jnp.concatenate([sum_of(("U", b, 0, c)) for c in range(4)], axis=1)
        res[0][b] = fine(fine(invs[0][b], grad, 1, 0), invs[1][b], 1, 0)

    def precondition_down(b):
        grad = jnp.concatenate([sum_of(("D", b, 0, c)) for c in range(4)], axis=1)
        res[1][b] = fine(invs[3][b], fine(grad, invs[2][b], 1, 1), 0, 0).T

    tick(2, 1)
    symmetric("H", 2, 0)
    tick(2, 2)
    tick(1, 4)
    tick(2, 3)
    symmetric("H", 2, 1)
    tick(1, 5)
    narrow("A", 0, 0)
    narrow("Q", 3, 1)
    precondition_down(1)
    tick(2, 4)
    tick(1, 6)
    precondition_up(1)
    precondition_down(0)
    tick(2, 5)
    symmetric("S", 1, 1)
    narrow("A", 0, 1)
    narrow("Q", 3, 0)
    tick(2, 6)
    symmetric("S", 1, 0)
    precondition_up(0)
    for piece in range(len(PIECES)):
        for hop in range(3):
            for copy in share(piece, hop, 0) + share(piece, hop, 1):
                copy.wait_send()


def solution(mesh):
    axis_size = mesh.shape["data"]

    def local_step(tokens, out_grad, w_up, w_down, a_up_old, s_up_old, a_down_old, s_down_old,
                   a_up_inv, s_up_inv, a_down_inv, s_down_inv, factor_decay):
        rows = tokens.shape[0]
        count = rows // (2 * TILE)
        small, wide = (2, LANES, LANES), (2, WIDE, WIDE)
        out_shapes = ((2, LANES, WIDE), (2, WIDE, LANES), small, wide, wide, small)

        def kernel(tok, og, wu, wd, rho, *refs):
            body(axis_size, rows, tok, og, wu, wd, rho, refs[0:4], refs[4:8], refs[8:10], refs[10:14],
                 *refs[14:23], refs[23:25], *refs[25:34], refs[34:38], *refs[38:])

        anywhere = pl.BlockSpec(memory_space=pl.ANY)
        inside = pl.BlockSpec(memory_space=pltpu.VMEM)
        half = lambda *shape: pltpu.VMEM(shape, BF)
        full = lambda *shape: pltpu.VMEM(shape, F32)
        sems = pltpu.SemaphoreType.DMA
        found = pl.pallas_call(
            kernel,
            in_specs=[anywhere] * 4 + [pl.BlockSpec(memory_space=pltpu.SMEM)] + [anywhere] * 8,
            out_specs=[inside] * 6,
            out_shape=[full(*s) for s in out_shapes],
            scratch_shapes=[half(rows, LANES), half(rows, LANES), half(2, LANES, WIDE), half(2, WIDE, LANES), half(WIDE, rows), half(WIDE, rows), half(WIDE, rows), half(LANES, rows),
                            half(LANES, rows), half(1280, TILE), half(1280, TILE), half(2, WIDE, LANES), half(LANES, WIDE),
                            full(2, 640, 256), full(2, 384, 256), full(256, 256), full(LANES, WIDE),
                            full(TOTAL_ROWS, LANES), full(TOTAL_ROWS - TOTAL_ROWS // 16, LANES), full(TOTAL_ROWS, LANES)]
            + [full(*s) for s in out_shapes[2:]]
            + [sems((2 * count + 10,)), sems((2, 5, len(PIECES))), sems((2, 5, len(PIECES)))],
            compiler_params=pltpu.CompilerParams(vmem_limit_bytes=57 * 2**20, collective_id=0, has_side_effects=True),
        )(tokens, out_grad, w_up, w_down, factor_decay.reshape(1), a_up_old, s_up_old, a_down_old, s_down_old,
          a_up_inv, s_up_inv, a_down_inv, s_down_inv)

        def put_out(*refs):
            stores = [pltpu.make_async_copy(refs[n], refs[6 + n], refs[12].at[n]) for n in range(6)]
            for store in stores:
                store.start()
            for store in stores:
                store.wait()

        return tuple(pl.pallas_call(
            put_out,
            in_specs=[inside] * 6,
            out_specs=[anywhere] * 6,
            out_shape=[jax.ShapeDtypeStruct(s, F32) for s in out_shapes],
            scratch_shapes=[sems((6,))],
            compiler_params=pltpu.CompilerParams(vmem_limit_bytes=2**20),
        )(*[pltpu.with_memory_space_constraint(x, pltpu.VMEM) for x in found]))

    batch_spec = P("data", None)
    return jax.shard_map(local_step, mesh=mesh, in_specs=(batch_spec, batch_spec) + (P(),) * 11,
                         out_specs=(P(),) * 6, check_vma=False)
```
